16 devices in a mesh: dp: 16 (over z, y, x, core).
Axes of the slice: x: 2, y: 2, z: 2, core: 2. Of those that a mesh axis runs over, the one named last changes fastest.
Arguments:
- features: bfloat16 [4096, 256], P('dp')
- w_in: bfloat16 [256, 1024], replicated
- w_out: bfloat16 [1024, 128], replicated
- item_table: bfloat16 [262144, 128], P('dp')
- cand_ids: int32 [16384], replicated
- log_q: float32 [16384], replicated
- targets: int32 [4096], P('dp')
Outputs:
- output 1: float32 [], replicated
- output 2: float32 [262144, 128], P('dp')
- output 3: float32 [256, 1024], replicated
- output 4: float32 [1024, 128], replicated
All inputs are finite; a program needn't handle non-finite values.
Results may differ from the reference program's by a relative error of at most 0.001.
Values are sent between devices in bfloat16 or wider.
A program may use at most 1 GiB of HBM per device.

```python
import jax
import jax.numpy as jnp
from jax import lax

IN_DIM = 256
HID_DIM = 1024
EMB_DIM = 128
NUM_ITEMS = 262144
GROUPS = 16
TOK_DEV = 256
CAND_DEV = 1024
TOKENS = 4096
NUM_CANDS = 16384
BLOCK_ROWS = 16384


def draw_ids(id_key):
    key_perm, key_blk_a, key_blk_b, key_hit, key_row = jax.random.split(id_key, 5)
    perm_keys = jax.random.split(key_perm, GROUPS)
    local_rows = jax.vmap(lambda perm_key: jax.random.permutation(perm_key, BLOCK_ROWS)[:CAND_DEV])(perm_keys)
    block_base = BLOCK_ROWS * jnp.arange(GROUPS, dtype=jnp.int32)
    cand_ids = (local_rows.astype(jnp.int32) + block_base[:, None]).reshape(NUM_CANDS)
    tok_pos = jnp.arange(TOKENS, dtype=jnp.int32)
    skew_block = jnp.minimum(jax.random.randint(key_blk_a, (TOKENS,), 0, GROUPS), jax.random.randint(key_blk_b, (TOKENS,), 0, GROUPS))
    owner_block = jnp.where(tok_pos < GROUPS, tok_pos, skew_block)
    hit_slot = owner_block * CAND_DEV + jax.random.randint(key_hit, (TOKENS,), 0, CAND_DEV)
    row_pair = jax.random.randint(key_row, (2, TOKENS), 0, BLOCK_ROWS)
    plain_row = owner_block * BLOCK_ROWS + jnp.minimum(row_pair[0], row_pair[1])
    targets = jnp.where(tok_pos % 4 == 1, cand_ids[hit_slot], plain_row)
    return cand_ids, targets.astype(jnp.int32)


def setup_inputs(seed: int = 0) -> dict:
    root_key = jax.random.key(seed)
    key_x, key_w1, key_w2, key_tab, key_lq, key_ids = jax.random.split(root_key, 6)
    cand_ids, targets = draw_ids(key_ids)
    features = jax.random.normal(key_x, (TOKENS, IN_DIM), jnp.float32).astype(jnp.bfloat16)
    w_in = (jax.random.normal(key_w1, (IN_DIM, HID_DIM), jnp.float32) * IN_DIM ** -0.5).astype(jnp.bfloat16)
    w_out = (jax.random.normal(key_w2, (HID_DIM, EMB_DIM), jnp.float32) * HID_DIM ** -0.5).astype(jnp.bfloat16)
    item_table = (jax.random.normal(key_tab, (NUM_ITEMS, EMB_DIM), jnp.float32) * (2.0 * EMB_DIM ** -0.5)).astype(jnp.bfloat16)
    log_q = jax.random.uniform(key_lq, (NUM_CANDS,), jnp.float32, -4.0, 0.0)
    return {"features": features, "w_in": w_in, "w_out": w_out, "item_table": item_table, "cand_ids": cand_ids, "log_q": log_q, "targets": targets}


def reference(features, w_in, w_out, item_table, cand_ids, log_q, targets):
    cand_rows = item_table[cand_ids]
    feat_blocks = features.reshape(GROUPS, TOK_DEV, IN_DIM)
    tgt_blocks = targets.reshape(GROUPS, TOK_DEV)

    def block_step(carry, block_in):
        grad_cand, grad_w_in, grad_w_out, loss_sum = carry
        feat_blk, tgt_blk = block_in
        pre_act = jnp.dot(feat_blk, w_in, preferred_element_type=jnp.float32)
        act_val, gelu_back = jax.vjp(jax.nn.gelu, pre_act)
        act_b = act_val.astype(jnp.bfloat16)
        query = jnp.dot(act_b, w_out, preferred_element_type=jnp.float32).astype(jnp.bfloat16)
        query_f = query.astype(jnp.float32)
        tgt_rows = item_table[tgt_blk].astype(jnp.float32)
        tgt_logit = jnp.sum(query_f * tgt_rows, axis=1)
        cand_logit = jnp.dot(query, cand_rows.T, preferred_element_type=jnp.float32) - log_q[None, :]
        cand_logit = jnp.where(cand_ids[None, :] == tgt_blk[:, None], -1e9, cand_logit)
        top_val = jnp.maximum(jnp.max(cand_logit, axis=1), tgt_logit)
        exp_sum = jnp.sum(jnp.exp(cand_logit - top_val[:, None]), axis=1) + jnp.exp(tgt_logit - top_val)
        log_norm = top_val + jnp.log(exp_sum)
        grad_tgt = (jnp.exp(tgt_logit - log_norm) - 1.0) / TOKENS
        cand_grad = (jnp.exp(cand_logit - log_norm[:, None]) / TOKENS).astype(jnp.bfloat16)
        d_query = (grad_tgt[:, None] * tgt_rows + jnp.dot(cand_grad, cand_rows, preferred_element_type=jnp.float32)).astype(jnp.bfloat16)
        d_act = jnp.dot(d_query, w_out.T, preferred_element_type=jnp.float32)
        d_pre = gelu_back(d_act)[0].astype(jnp.bfloat16)
        grad_cand = grad_cand + jnp.dot(cand_grad.T, query, preferred_element_type=jnp.float32)
        grad_w_in = grad_w_in + jnp.dot(feat_blk.T, d_pre, preferred_element_type=jnp.float32)
        grad_w_out = grad_w_out + jnp.dot(act_b.T, d_query, preferred_element_type=jnp.float32)
        loss_sum = loss_sum + jnp.sum(log_norm - tgt_logit)
        return (grad_cand, grad_w_in, grad_w_out, loss_sum), grad_tgt[:, None] * query_f

    start_carry = (jnp.zeros((NUM_CANDS, EMB_DIM), jnp.float32), jnp.zeros((IN_DIM, HID_DIM), jnp.float32), jnp.zeros((HID_DIM, EMB_DIM), jnp.float32), jnp.zeros((), jnp.float32))
    end_carry, tgt_grad = lax.scan(block_step, start_carry, (feat_blocks, tgt_blocks))
    grad_cand, grad_w_in, grad_w_out, loss_sum = end_carry
    grad_table = jnp.zeros((NUM_ITEMS, EMB_DIM), jnp.float32).at[cand_ids].add(grad_cand).at[targets].add(tgt_grad.reshape(TOKENS, EMB_DIM))
    return loss_sum / TOKENS, grad_table, grad_w_in, grad_w_out
```

```python
import jax
import jax.numpy as jnp
from jax import lax
from jax.experimental import pallas as pl
from jax.experimental.pallas import tpu as pltpu
from jax.sharding import PartitionSpec as P

F32 = jnp.float32
BF16 = jnp.bfloat16
I32 = jnp.int32
MESH = pl.DeviceIdType.MESH

CORES = 2
CHIPS = 8
DEVS = 16
LANES = 128
TOK = 256
HALF = 128
GRP = 2048
CAND = 1024
PAIR = 2048
CROW = 8
EMB = 128
HID = 1024
IN = 256
ROWS = 16384
TOTAL = 4096
KC = 256
STEPS = PAIR // KC
HB = 256
HSTEPS = HID // HB
ROOT_2_PI = 0.7978845608028654
CUBE = 0.044715
SHARE = 1.0 / TOTAL
VMEM_LIMIT = 64 * 1024 * 1024 - 65536

NEAR = (1, 2, 4, 3, 5, 6, 7)
FAR = (7, 6, 5, 3, 4, 2, 1)


def dot_nt(lhs, rhs):
    return lax.dot_general(lhs, rhs, (((1,), (1,)), ((), ())), preferred_element_type=F32)


def dot_nn(lhs, rhs):
    return jnp.dot(lhs, rhs, preferred_element_type=F32)


def column_of(row):
    return jnp.broadcast_to(row, (LANES, LANES)).T


def top_of(x):
    return jnp.max(x, axis=0, keepdims=True)


def sum_of(x):
    return jnp.sum(x, axis=0, keepdims=True)


def part(i, size):
    return pl.ds(pl.multiple_of(i * size, size), size)


def row(i):
    return pl.ds(i, 1)


def tanh_of(act):
    return jnp.tanh(ROOT_2_PI * (act + CUBE * (act * act * act)))


def main_kernel(
    x_ref, w_in_ref, w_out_ref, tgt_ref, cand_hbm, logq_hbm, table_hbm,
    loss_out, gcand_out, gh_out, idx_out, bounds_out, dwin_out, dwout_out,
    tab_b, tab_f, tall, idx_vm, idx_sm, cand_vm, logq_vm, xs_all, xt_ref, u_ref, hall,
    rows_f, cand_f, e_all, e_t, cid_b, lq_b, trow_s, trow_o, tr_t,
    ex_ref, st_all, mloc_ref, z_ref, l_ref, f_ref, g_ref, gh_ref,
    dh_acc, dh_in, dhb_all, da_ref, de_acc, de_in, gwin, gwout, swin, swout, loss_all, bounds_vm,
    tgt_s, tgt_r, h_s, h_r, x_s, x_r, e_s, e_r, tr_s, tr_r, st_s, st_r, dh_s, dh_r, de_s, de_r, gh_s, gh_r,
    db_s, db_r, wi_s, wi_r, wo_s, wo_r, ls_s, ls_r, loc,
):
    me = lax.axis_index("dp")
    chip = me // CORES
    core = me % CORES
    oth = 1 - core
    sib = chip * CORES + oth
    base = me * ROWS
    first_row = chip * (CORES * ROWS)

    def flip(k):
        out = 0
        for bit in (1, 2, 4):
            out = out + (((chip // bit) + (k // bit)) % 2) * bit
        return out

    peers = {k: flip(k) for k in NEAR}

    def slot_of(device):
        return (device % CORES) * CHIPS + device // CORES

    def rcopy(src, dst, ssem, rsem, dev):
        return pltpu.make_async_remote_copy(src_ref=src, dst_ref=dst, send_sem=ssem, recv_sem=rsem, device_id=(dev,), device_id_type=MESH)

    sent = []

    def go(copy):
        copy.start()
        sent.append(copy)
        return copy

    def swap(src, dst, ssem, rsem):
        return go(rcopy(src, dst, ssem, rsem, sib))

    def arrivals(ref, ssem, rsem):
        return {k: rcopy(ref.at[src], ref.at[src], ssem.at[k], rsem.at[src], src * CORES + core) for k, src in peers.items()}

    def spread(ref, ssem, rsem, ks):
        got = arrivals(ref, ssem, rsem)
        for k in ks:
            go(rcopy(ref.at[chip], ref.at[chip], ssem.at[k], rsem.at[chip], peers[k] * CORES + core))
        return got

    def to_all(ref, slot, ssem, rsem, slots):
        got = []
        for i in range(DEVS - 1):
            src = slots(lax.rem(me + (DEVS - 1) - i, DEVS))
            got.append(rcopy(ref.at[src], ref.at[src], ssem.at[i], rsem.at[src], others[i]))
        for i, dev in enumerate(others):
            go(rcopy(ref.at[slot], ref.at[slot], ssem.at[i], rsem.at[slot], dev))
        return got

    others = [lax.rem(me + k, DEVS) for k in range(1, DEVS)]

    barrier = pltpu.get_barrier_semaphore()
    for dev in others:
        pl.semaphore_signal(barrier, inc=1, device_id=(dev,), device_id_type=MESH)

    chip_blocks = pl.ds(chip * CORES, CORES)
    early = [
        pltpu.make_async_copy(cand_hbm.at[chip_blocks], cand_vm, loc.at[0]),
        pltpu.make_async_copy(logq_hbm.at[chip_blocks], logq_vm, loc.at[1]),
        pltpu.make_async_copy(table_hbm, tab_b, loc.at[2]),
    ]
    for c in early:
        c.start()

    lane = lax.broadcasted_iota(I32, (1, LANES), 1)
    halves = range(TOK // HALF)
    tgt = [tgt_ref[q:q + 1, :] for q in halves]
    key = [tgt[q] * TOK + (lane + q * HALF) for q in halves]
    key_col = [column_of(k) for k in key]
    sub = lax.broadcasted_iota(I32, (TOK, LANES), 0)
    hot = [sub == sum(sum_of((key_col[r] < key[q]).astype(I32)) for r in halves) for q in halves]
    perm = jnp.concatenate([jnp.where(h, 1.0, 0.0).astype(BF16) for h in hot], axis=1)
    moved = [jnp.where(hot[q], jnp.broadcast_to(tgt[q].astype(F32), (TOK, LANES)), 0.0) for q in halves]
    my_slot = core * CHIPS + chip
    for r in halves:
        line = sum(sum_of(m[r * HALF:(r + 1) * HALF, :].T) for m in moved)
        tall[row(my_slot), row(r), :] = line.astype(I32).reshape(1, 1, LANES)

    pl.semaphore_wait(barrier, DEVS - 1)
    tgt_got = to_all(tall, my_slot, tgt_s, tgt_r, slot_of)

    xs = dot_nn(perm, x_ref[...]).astype(BF16)
    xs_all[row(chip)] = xs.reshape(1, TOK, IN)
    act = dot_nn(xs, w_in_ref[...])
    u_ref[...] = (act * (0.5 * (1.0 + tanh_of(act)))).astype(BF16)
    hall[row(chip)] = dot_nn(u_ref[...], w_out_ref[...]).astype(BF16).reshape(1, TOK, EMB)
    h_got = spread(hall, h_s, h_r, NEAR)
    x_got = spread(xs_all, x_s, x_r, NEAR)

    for c in early:
        c.wait()
    for r in range(CROW):
        idx_vm[DEVS + r // 2, r % 2:r % 2 + 1, :] = jnp.clip(cand_vm[core, r:r + 1, :] - base, 0, ROWS - 1)
    cand_at = pl.ds(DEVS, CROW // 2)
    cand_copy = pltpu.make_async_copy(idx_vm.at[cand_at], idx_sm.at[cand_at], loc.at[0])
    cand_copy.start()

    @pl.loop(0, ROWS // KC)
    def _(i):
        tab_f[part(i, KC), :] = tab_b[part(i, KC), :].astype(F32)

    tab_f[pl.ds(ROWS, CROW), :] = jnp.zeros((CROW, EMB), F32)
    cand_copy.wait()

    def gather_rows(slot, dst, first):
        for v in range(TOK):
            dst[row(first + v), :] = tab_f[row(idx_sm[slot, v // LANES, v % LANES]), :]

    @pl.loop(0, CAND // TOK)
    def _(i):
        gather_rows(DEVS + i, cand_f, i * TOK)

    e_all[row(core)] = cand_f[...].astype(BF16).reshape(1, CAND, EMB)
    e_copy = swap(e_all.at[core], e_all.at[core], e_s, e_r)

    for c in tgt_got:
        c.wait_recv()
    loc_idx = tall[...] - base
    own = (loc_idx >= 0) & (loc_idx < ROWS)
    idx_vm[0:DEVS] = jnp.where(own, loc_idx, ROWS)

    def count(mask):
        return jnp.sum(jnp.sum(mask.astype(F32), axis=2, keepdims=True), axis=1, keepdims=True)

    lane3 = lax.broadcasted_iota(I32, (DEVS, 1, LANES), 2)
    bounds_vm[...] = jnp.where(lane3 == 0, count(loc_idx < 0), count(loc_idx < ROWS)).astype(I32)
    tok_at = pl.ds(0, DEVS)
    idx_copy = pltpu.make_async_copy(idx_vm.at[tok_at], idx_sm.at[tok_at], loc.at[0])
    idx_copy.start()
    idx_copy.wait()

    @pl.loop(0, CHIPS)
    def _(q):
        gather_rows(oth * CHIPS + q, rows_f, q * TOK)

    trow_s[...] = rows_f[...].astype(BF16)
    tr_copy = swap(trow_s, trow_o, tr_s, tr_r)

    @pl.loop(0, CHIPS)
    def _(q):
        gather_rows(core * CHIPS + q, rows_f, q * TOK)

    for b in range(CORES):
        for r in range(CROW):
            at = b * CAND + r * LANES
            cid_b[at:at + LANES, :] = column_of(cand_vm[b, r:r + 1, :])
            lq_b[at:at + LANES, :] = column_of(logq_vm[b, r:r + 1, :])
    e_copy.wait_recv()
    for i in range(STEPS):
        b, r = i // (CAND // KC), i % (CAND // KC)
        e_t[:, i * KC:(i + 1) * KC] = e_all[b, r * KC:(r + 1) * KC, :].T
    tr_copy.wait_recv()

    def twice(x):
        return jnp.concatenate([x, x], axis=1)

    def fold(x):
        return x.reshape(KC // 8, 8, TOK)

    def stats_of(q):
        h = hall[q]
        ids = tall[core * CHIPS + q]
        y_row = jnp.concatenate([ids[r:r + 1, :] for r in halves], axis=1)

        def first(i, top):
            e_blk = e_all[i // (CAND // KC), part(i % (CAND // KC), KC), :]
            s = dot_nt(e_blk, h) - twice(lq_b[part(i, KC), :])
            s = jnp.where(twice(cid_b[part(i, KC), :]) == y_row, -1e9, s)
            ex_ref[q, part(i, KC), :] = s
            return jnp.maximum(top, jnp.max(fold(s), axis=0))

        top = top_of(lax.fori_loop(0, STEPS, first, jnp.full((8, TOK), -jnp.inf, F32)))

        def second(i, tot):
            e = jnp.exp(ex_ref[q, part(i, KC), :] - top)
            ex_ref[q, part(i, KC), :] = e
            return tot + jnp.sum(fold(e), axis=0)

        tot = sum_of(lax.fori_loop(0, STEPS, second, jnp.zeros((8, TOK), F32)))
        rows = rows_f[part(q, TOK), :] + trow_o[part(q, TOK), :].astype(F32)
        tr_t[q] = rows.T
        z = sum_of((rows * h.astype(F32)).T)
        mine = (y_row >= first_row) & (y_row < first_row + CORES * ROWS)
        z_ref[row(q), :] = jnp.where(mine, z, 0.0)
        both = jnp.where(mine, jnp.maximum(top, z), top)
        tot = tot * jnp.exp(top - both) + jnp.where(mine, jnp.exp(jnp.where(mine, z - both, 0.0)), 0.0)
        mloc_ref[row(q), :] = top
        st_all[row(chip), 0, row(q), :] = both.reshape(1, 1, TOK)
        st_all[row(chip), 1, row(q), :] = tot.reshape(1, 1, TOK)

    stats_of(chip)
    for k in NEAR:
        h_got[k].wait_recv()
        stats_of(peers[k])
    st_got = spread(st_all, st_s, st_r, FAR)

    def tower_of(q):
        x = xs_all[q]
        xt_ref[:, part(q, TOK)] = x.T

        def step(i, carry):
            act = dot_nn(x, w_in_ref[:, part(i, HB)])
            tanh = tanh_of(act)
            cdf = 0.5 * (1.0 + tanh)
            slope = cdf + act * (0.5 * (1.0 - tanh * tanh)) * (ROOT_2_PI * (1.0 + 3.0 * CUBE * (act * act)))
            u_t = (act * cdf).T.astype(BF16)
            for r in halves:
                at = (q * HSTEPS + i) * 2 + r
                tab_f[part(at, TOK), :] = slope[:, r * HALF:(r + 1) * HALF]
                tab_b[part(at, HB), :] = u_t[:, r * HALF:(r + 1) * HALF]
            return carry

        lax.fori_loop(0, HSTEPS, step, 0)

    tower_of(chip)
    for k in NEAR[:3]:
        x_got[k].wait_recv()
        tower_of(peers[k])

    for k in NEAR:
        st_got[k].wait_recv()
    top_all = st_all[0, 0]
    for c in range(1, CHIPS):
        top_all = jnp.maximum(top_all, st_all[c, 0])
    tot_all = sum(st_all[c, 1] * jnp.exp(st_all[c, 0] - top_all) for c in range(CHIPS))
    log_norm = top_all + jnp.log(tot_all)
    l_ref[...] = log_norm
    f_ref[...] = jnp.exp(mloc_ref[...] - log_norm) * SHARE
    group = pl.ds(core * CHIPS, CHIPS)
    t_all = jnp.concatenate([tall[group, r, :] for r in halves], axis=1)
    mine_all = (t_all >= first_row) & (t_all < first_row + CORES * ROWS)
    z_all = z_ref[...]
    g_ref[...] = jnp.where(mine_all, (jnp.exp(jnp.where(mine_all, z_all - log_norm, 0.0)) - 1.0) * SHARE, 0.0)
    loss_all[row(me)] = (l_ref[row(chip), :] - sum_of(z_all)).reshape(1, 1, TOK)
    ls_got = to_all(loss_all, me, ls_s, ls_r, lambda device: device)

    def grads_of(q, is_first):
        h = hall[q]
        f_row = f_ref[row(q), :]

        def body(i, acc):
            p = (ex_ref[q, part(i, KC), :] * f_row).astype(BF16)
            de = dot_nn(p, h)
            if is_first:
                de_acc[part(i, KC), :] = de
            else:
                de_acc[part(i, KC), :] += de
            return acc + dot_nn(e_t[:, part(i, KC)], p)

        dh_acc[q] = lax.fori_loop(0, STEPS, body, g_ref[row(q), :] * tr_t[q])

    dh_got = arrivals(dh_in, dh_s, dh_r)
    for k in FAR:
        grads_of(peers[k], k == FAR[0])
        go(rcopy(dh_acc.at[peers[k]], dh_in.at[chip], dh_s.at[k], dh_r.at[chip], peers[k] * CORES + core))
    grads_of(chip, False)
    de_copy = swap(de_acc.at[part(oth, CAND), :], de_in, de_s, de_r)

    @pl.loop(0, CHIPS)
    def _(q):
        g_row = g_ref[row(q), :]
        for r in halves:
            col = column_of(g_row[:, r * HALF:(r + 1) * HALF])
            gh_ref[part((core * CHIPS + q) * 2 + r, HALF), :] = col * hall[q, r * HALF:(r + 1) * HALF, :].astype(F32)

    gh_copy = swap(gh_ref.at[part(core, GRP), :], gh_ref.at[part(core, GRP), :], gh_s, gh_r)

    for k in NEAR[3:]:
        x_got[k].wait_recv()
        tower_of(peers[k])

    de_copy.wait_recv()
    for r in range(CAND // KC):
        cand_f[r * KC:(r + 1) * KC, :] = de_acc[part(core * (CAND // KC) + r, KC), :] + de_in[r * KC:(r + 1) * KC, :]
    for c in ls_got:
        c.wait_recv()
    loss_out[...] = jnp.sum(jnp.sum(loss_all[...], axis=0), axis=1, keepdims=True) * SHARE
    gh_copy.wait_recv()
    outs = [
        pltpu.make_async_copy(gh_ref, gh_out, loc.at[0]),
        pltpu.make_async_copy(idx_vm, idx_out, loc.at[1]),
        pltpu.make_async_copy(bounds_vm, bounds_out, loc.at[2]),
        pltpu.make_async_copy(cand_f, gcand_out, loc.at[3]),
    ]
    for c in outs:
        c.start()

    for k in NEAR:
        dh_got[k].wait_recv()
    total = dh_acc[chip]
    for k in NEAR:
        total = total + dh_in[peers[k]]
    dhb_all[row(chip)] = total.T.astype(BF16).reshape(1, TOK, EMB)
    db_got = spread(dhb_all, db_s, db_r, FAR)

    def back_of(q):
        dh = dhb_all[q]

        def step(i, carry):
            e = dot_nt(dh, w_out_ref[part(i, HB), :])
            slope = [tab_f[part((q * HSTEPS + i) * 2 + r, TOK), :] for r in halves]
            da_ref[part(q, TOK), part(i, HB)] = (jnp.concatenate(slope, axis=1) * e).astype(BF16)
            return carry

        lax.fori_loop(0, HSTEPS, step, 0)

    back_of(chip)
    for k in FAR:
        db_got[k].wait_recv()
        back_of(peers[k])

    w_got = []
    for i in range(HSTEPS):
        gwin[i] = dot_nn(xt_ref[...], da_ref[:, i * HB:(i + 1) * HB])
        w_got.append(swap(gwin.at[i], swin.at[i], wi_s.at[i], wi_r.at[i]))
    dh_flat = dhb_all[...].reshape(GRP, EMB)
    for i in range(HSTEPS):
        u_t = jnp.concatenate([tab_b[((q * HSTEPS + i) * 2 + r) * HB:((q * HSTEPS + i) * 2 + r + 1) * HB, :] for q in range(CHIPS) for r in halves], axis=1)
        gwout[i * HB:(i + 1) * HB, :] = dot_nn(u_t, dh_flat)
    w_got.append(swap(gwout, swout, wo_s, wo_r))
    for i in range(HSTEPS):
        w_got[i].wait_recv()
        w_got[i].wait_send()
        gwin[i] += swin[i]
        outs.append(pltpu.make_async_copy(gwin.at[i], dwin_out.at[:, part(i, HB)], loc.at[4 + i]))
        outs[-1].start()
    w_got[-1].wait_recv()
    w_got[-1].wait_send()
    gwout[...] += swout[...]
    outs.append(pltpu.make_async_copy(gwout, dwout_out, loc.at[4 + HSTEPS]))
    outs[-1].start()

    for c in sent:
        if not any(c is w for w in w_got):
            c.wait_send()
    for c in outs:
        c.wait()


def scatter_kernel(gcand_hbm, gh_hbm, idx_hbm, bounds_hbm, dwin_ref, dwout_ref, grad_out, dwin_out, dwout_out, acc, gcand, gh, idx_sm, bounds_sm, win_b, wout_b, sems):
    ins = [
        pltpu.make_async_copy(src, dst, sems.at[i])
        for i, (src, dst) in enumerate([(idx_hbm, idx_sm), (bounds_hbm, bounds_sm), (gcand_hbm, gcand), (gh_hbm, gh), (dwin_ref, win_b), (dwout_ref, wout_b)])
    ]
    for c in ins:
        c.start()

    @pl.loop(0, ROWS // KC)
    def _(i):
        acc[part(i, KC), :] = jnp.zeros((KC, EMB), F32)

    for c in ins[:3]:
        c.wait()

    @pl.loop(0, CAND // LANES)
    def _(i):
        for v in range(LANES):
            acc[row(idx_sm[DEVS + i // 2, i % 2, v]), :] = gcand[row(i * LANES + v), :]

    for c in ins[3:]:
        c.wait()
    outs = [pltpu.make_async_copy(win_b, dwin_out, sems.at[6]), pltpu.make_async_copy(wout_b, dwout_out, sems.at[7])]
    for c in outs:
        c.start()

    @pl.loop(0, DEVS)
    def _(s):
        def add(i, carry):
            for v in range(CROW):
                r = idx_sm[s, i >> 4, (i & 15) * CROW + v]
                acc[row(r), :] += gh[row(s * TOK + i * CROW + v), :]
            return carry

        lax.fori_loop(bounds_sm[s, 0, 0] >> 3, (bounds_sm[s, 0, 1] + 7) >> 3, add, 0)

    outs.append(pltpu.make_async_copy(acc.at[pl.ds(0, ROWS), :], grad_out, sems.at[8]))
    outs[-1].start()
    for c in outs:
        c.wait()


def solution(mesh):
    def local_step(features, w_in, w_out, table_blk, cand_ids, log_q, targets):
        vmem = pl.BlockSpec(memory_space=pltpu.VMEM)
        hbm = pl.BlockSpec(memory_space=pl.ANY)
        dma = pltpu.SemaphoreType.DMA
        sds = jax.ShapeDtypeStruct

        def v(dtype, *shape):
            return pltpu.VMEM(shape, dtype)

        chips = dma((CHIPS,))
        idx_shape = (DEVS + CROW // 2, 2, LANES)
        loss, gcand, gh, idx, bounds, dwin, dwout = pl.pallas_call(
            main_kernel,
            name="main_kernel",
            out_shape=(
                sds((1, 1), F32), sds((CAND, EMB), F32), sds((TOTAL, EMB), F32),
                sds(idx_shape, I32), sds((DEVS, 1, LANES), I32), sds((IN, HID), F32), sds((HID, EMB), F32),
            ),
            in_specs=[vmem] * 4 + [hbm] * 3,
            out_specs=(vmem,) + (hbm,) * 6,
            scratch_shapes=[
                v(BF16, ROWS, EMB),
                v(F32, ROWS + CROW, EMB),
                v(I32, DEVS, 2, LANES),
                v(I32, *idx_shape),
                pltpu.SMEM(idx_shape, I32),
                v(I32, CORES, CROW, LANES),
                v(F32, CORES, CROW, LANES),
                v(BF16, CHIPS, TOK, IN),
                v(BF16, IN, GRP),
                v(BF16, TOK, HID),
                v(BF16, CHIPS, TOK, EMB),
                v(F32, GRP, EMB),
                v(F32, CAND, EMB),
                v(BF16, CORES, CAND, EMB),
                v(BF16, EMB, PAIR),
                v(I32, PAIR, LANES),
                v(F32, PAIR, LANES),
                v(BF16, GRP, EMB),
                v(BF16, GRP, EMB),
                v(F32, CHIPS, EMB, TOK),
                v(F32, CHIPS, PAIR, TOK),
                v(F32, CHIPS, 2, CHIPS, TOK),
                v(F32, CHIPS, TOK),
                v(F32, CHIPS, TOK),
                v(F32, CHIPS, TOK),
                v(F32, CHIPS, TOK),
                v(F32, CHIPS, TOK),
                v(F32, TOTAL, EMB),
                v(F32, CHIPS, EMB, TOK),
                v(F32, CHIPS, EMB, TOK),
                v(BF16, CHIPS, TOK, EMB),
                v(BF16, GRP, HID),
                v(F32, PAIR, EMB),
                v(F32, CAND, EMB),
                v(F32, HSTEPS, IN, HB),
                v(F32, HID, EMB),
                v(F32, HSTEPS, IN, HB),
                v(F32, HID, EMB),
                v(F32, DEVS, 1, TOK),
                v(I32, DEVS, 1, LANES),
                dma((DEVS - 1,)), dma((DEVS,)),
                chips, chips,
                chips, chips,
                dma, dma,
                dma, dma,
                chips, chips,
                chips, chips,
                dma, dma,
                dma, dma,
                chips, chips,
                dma((HSTEPS,)), dma((HSTEPS,)),
                dma, dma,
                dma((DEVS - 1,)), dma((DEVS,)),
                dma((CROW + HSTEPS,)),
            ],
            compiler_params=pltpu.CompilerParams(collective_id=0, has_side_effects=True, vmem_limit_bytes=VMEM_LIMIT),
        )(features, w_in, w_out, targets.reshape(2, LANES), cand_ids.reshape(DEVS, CROW, LANES), log_q.reshape(DEVS, CROW, LANES), table_blk)
        grad_blk, grad_in, grad_out = pl.pallas_call(
            scatter_kernel,
            name="scatter_kernel",
            out_shape=(sds((ROWS, EMB), F32), sds((IN, HID), F32), sds((HID, EMB), F32)),
            in_specs=[hbm] * 6,
            out_specs=(hbm,) * 3,
            scratch_shapes=[
                v(F32, ROWS + CROW, EMB),
                v(F32, CAND, EMB),
                v(F32, TOTAL, EMB),
                pltpu.SMEM(idx_shape, I32),
                pltpu.SMEM((DEVS, 1, LANES), I32),
                v(F32, IN, HID),
                v(F32, HID, EMB),
                dma((9,)),
            ],
            compiler_params=pltpu.CompilerParams(vmem_limit_bytes=VMEM_LIMIT),
        )(gcand, gh, idx, bounds, dwin, dwout)
        return loss[0, 0], grad_blk, grad_in, grad_out

    return jax.shard_map(local_step, mesh=mesh, in_specs=(P("dp", None), P(), P(), P("dp", None), P(), P(), P("dp")), out_specs=(P(), P("dp", None), P(), P()), check_vma=False)
```

```python
import jax
import jax.numpy as jnp
from jax import lax
from jax.experimental import pallas as pl
from jax.experimental.pallas import tpu as pltpu
from jax.sharding import PartitionSpec as P

F32 = jnp.float32
BF16 = jnp.bfloat16
I32 = jnp.int32
MESH = pl.DeviceIdType.MESH

CORES = 2
CHIPS = 8
DEVS = 16
LANES = 128
TOK = 256
HALF = 128
GRP = 2048
CAND = 1024
PAIR = 2048
CROW = 8
EMB = 128
HID = 1024
IN = 256
ROWS = 16384
TOTAL = 4096
KC = 256
HB = 256
HSTEPS = HID // HB
ROOT_2_PI = 0.7978845608028654
CUBE = 0.044715
SHARE = 1.0 / TOTAL
VMEM_LIMIT = 64 * 1024 * 1024 - 65536

NEAR = (1, 2, 4, 3, 5, 6, 7)
FAR = (7, 6, 5, 3, 4, 2, 1)


def dot_nt(lhs, rhs):
    return lax.dot_general(lhs, rhs, (((1,), (1,)), ((), ())), preferred_element_type=F32)


def dot_nn(lhs, rhs):
    return jnp.dot(lhs, rhs, preferred_element_type=F32)


def column_of(row):
    return jnp.broadcast_to(row, (LANES, LANES)).T


def top_of(x):
    return jnp.max(x, axis=0, keepdims=True)


def sum_of(x):
    return jnp.sum(x, axis=0, keepdims=True)


def part(i, size):
    return pl.ds(pl.multiple_of(i * size, size), size)


def row(i):
    return pl.ds(i, 1)


def tanh_of(act):
    return jnp.tanh(ROOT_2_PI * (act + CUBE * (act * act * act)))


def main_kernel(
    x_ref, w_in_ref, w_out_ref, tgt_ref, cand_hbm, logq_hbm, table_hbm,
    loss_out, gcand_out, gh_out, idx_out, bounds_out, dwin_out, dwout_out,
    tab_b, tab_f, tall, idx_vm, idx_sm, cand_vm, logq_vm, xs_all, xt_ref, u_ref, hall,
    rows_f, cand_f, e_all, e_t, cid_b, lq_b, trow_s, trow_o, tr_t,
    ex_ref, st_all, mloc_ref, z_ref, l_ref, f_ref, g_ref, gh_ref,
    dh_acc, dh_in, dhb_all, da_ref, de_acc, de_in, gwin, gwout, swin, swout, loss_all, bounds_vm,
    tgt_s, tgt_r, h_s, h_r, x_s, x_r, e_s, e_r, tr_s, tr_r, st_s, st_r, dh_s, dh_r, de_s, de_r, gh_s, gh_r,
    db_s, db_r, wi_s, wi_r, wo_s, wo_r, ls_s, ls_r, loc,
):
    me = lax.axis_index("dp")
    chip = me // CORES
    core = me % CORES
    oth = 1 - core
    sib = chip * CORES + oth
    base = me * ROWS
    first_row = chip * (CORES * ROWS)

    def flip(k):
        out = 0
        for bit in (1, 2, 4):
            out = out + (((chip // bit) + (k // bit)) % 2) * bit
        return out

    peers = {k: flip(k) for k in NEAR}

    def slot_of(device):
        return (device % CORES) * CHIPS + device // CORES

    def rcopy(src, dst, ssem, rsem, dev):
        return pltpu.make_async_remote_copy(src_ref=src, dst_ref=dst, send_sem=ssem, recv_sem=rsem, device_id=(dev,), device_id_type=MESH)

    sent = []

    def go(copy):
        copy.start()
        sent.append(copy)
        return copy

    def swap(src, dst, ssem, rsem):
        return go(rcopy(src, dst, ssem, rsem, sib))

    def arrivals(ref, ssem, rsem):
        return {k: rcopy(ref.at[src], ref.at[src], ssem.at[k], rsem.at[src], src * CORES + core) for k, src in peers.items()}

    def spread(ref, ssem, rsem, ks):
        got = arrivals(ref, ssem, rsem)
        for k in ks:
            go(rcopy(ref.at[chip], ref.at[chip], ssem.at[k], rsem.at[chip], peers[k] * CORES + core))
        return got

    def to_all(ref, slot, ssem, rsem, slots):
        got = []
        for i in range(DEVS - 1):
            src = slots(lax.rem(me + (DEVS - 1) - i, DEVS))
            got.append(rcopy(ref.at[src], ref.at[src], ssem.at[i], rsem.at[src], others[i]))
        for i, dev in enumerate(others):
            go(rcopy(ref.at[slot], ref.at[slot], ssem.at[i], rsem.at[slot], dev))
        return got

    others = [lax.rem(me + k, DEVS) for k in range(1, DEVS)]

    barrier = pltpu.get_barrier_semaphore()
    for dev in others:
        pl.semaphore_signal(barrier, inc=1, device_id=(dev,), device_id_type=MESH)

    chip_blocks = pl.ds(chip * CORES, CORES)
    early = [
        pltpu.make_async_copy(cand_hbm.at[chip_blocks], cand_vm, loc.at[0]),
        pltpu.make_async_copy(logq_hbm.at[chip_blocks], logq_vm, loc.at[1]),
        pltpu.make_async_copy(table_hbm, tab_b, loc.at[2]),
    ]
    for c in early:
        c.start()

    lane = lax.broadcasted_iota(I32, (1, LANES), 1)
    halves = range(TOK // HALF)
    tgt = [tgt_ref[q:q + 1, :] for q in halves]
    key = [tgt[q] * TOK + (lane + q * HALF) for q in halves]
    key_col = [column_of(k) for k in key]
    sub = lax.broadcasted_iota(I32, (TOK, LANES), 0)
    hot = [sub == sum(sum_of((key_col[r] < key[q]).astype(I32)) for r in halves) for q in halves]
    perm = jnp.concatenate([jnp.where(h, 1.0, 0.0).astype(BF16) for h in hot], axis=1)
    moved = [jnp.where(hot[q], jnp.broadcast_to(tgt[q].astype(F32), (TOK, LANES)), 0.0) for q in halves]
    my_slot = core * CHIPS + chip
    for r in halves:
        line = sum(sum_of(m[r * HALF:(r + 1) * HALF, :].T) for m in moved)
        tall[row(my_slot), row(r), :] = line.astype(I32).reshape(1, 1, LANES)

    pl.semaphore_wait(barrier, DEVS - 1)
    tgt_got = to_all(tall, my_slot, tgt_s, tgt_r, slot_of)

    xs = dot_nn(perm, x_ref[...]).astype(BF16)
    xs_all[row(chip)] = xs.reshape(1, TOK, IN)
    act = dot_nn(xs, w_in_ref[...])
    u_ref[...] = (act * (0.5 * (1.0 + tanh_of(act)))).astype(BF16)
    hall[row(chip)] = dot_nn(u_ref[...], w_out_ref[...]).astype(BF16).reshape(1, TOK, EMB)
    h_got = spread(hall, h_s, h_r, NEAR)
    x_got = spread(xs_all, x_s, x_r, NEAR)

    for c in early:
        c.wait()
    for r in range(CROW):
        idx_vm[DEVS + r // 2, r % 2:r % 2 + 1, :] = jnp.clip(cand_vm[core, r:r + 1, :] - base, 0, ROWS - 1)
    cand_at = pl.ds(DEVS, CROW // 2)
    cand_copy = pltpu.make_async_copy(idx_vm.at[cand_at], idx_sm.at[cand_at], loc.at[0])
    cand_copy.start()

    @pl.loop(0, ROWS // KC)
    def _(i):
        tab_f[part(i, KC), :] = tab_b[part(i, KC), :].astype(F32)

    tab_f[pl.ds(ROWS, CROW), :] = jnp.zeros((CROW, EMB), F32)
    cand_copy.wait()

    def gather_rows(slot, dst, first):
        for v in range(TOK):
            dst[row(first + v), :] = tab_f[row(idx_sm[slot, v // LANES, v % LANES]), :]

    @pl.loop(0, CAND // TOK)
    def _(i):
        gather_rows(DEVS + i, cand_f, i * TOK)

    e_all[row(core)] = cand_f[...].astype(BF16).reshape(1, CAND, EMB)
    e_copy = swap(e_all.at[core], e_all.at[core], e_s, e_r)

    for c in tgt_got:
        c.wait_recv()
    loc_idx = tall[...] - base
    own = (loc_idx >= 0) & (loc_idx < ROWS)
    idx_vm[0:DEVS] = jnp.where(own, loc_idx, ROWS)

    def count(mask):
        return jnp.sum(jnp.sum(mask.astype(F32), axis=2, keepdims=True), axis=1, keepdims=True)

    lane3 = lax.broadcasted_iota(I32, (DEVS, 1, LANES), 2)
    bounds_vm[...] = jnp.where(lane3 == 0, count(loc_idx < 0), count(loc_idx < ROWS)).astype(I32)
    tok_at = pl.ds(0, DEVS)
    idx_copy = pltpu.make_async_copy(idx_vm.at[tok_at], idx_sm.at[tok_at], loc.at[0])
    idx_copy.start()
    idx_copy.wait()

    @pl.loop(0, CHIPS)
    def _(q):
        gather_rows(oth * CHIPS + q, rows_f, q * TOK)

    trow_s[...] = rows_f[...].astype(BF16)
    tr_copy = swap(trow_s, trow_o, tr_s, tr_r)

    @pl.loop(0, CHIPS)
    def _(q):
        gather_rows(core * CHIPS + q, rows_f, q * TOK)

    for b in range(CORES):
        for r in range(CROW):
            at = b * CAND + r * LANES
            cid_b[at:at + LANES, :] = column_of(cand_vm[b, r:r + 1, :])
            lq_b[at:at + LANES, :] = column_of(logq_vm[b, r:r + 1, :])
    e_copy.wait_recv()
    for b in range(CORES):
        e_t[:, b * CAND:(b + 1) * CAND] = e_all[b].T
    tr_copy.wait_recv()

    def twice(x):
        return jnp.concatenate([x, x], axis=1)

    def fold(x):
        return x.reshape(PAIR // 8, 8, TOK)

    def stats_of(q):
        h = hall[q]
        ids = tall[core * CHIPS + q]
        y_row = jnp.concatenate([ids[r:r + 1, :] for r in halves], axis=1)

        s = dot_nt(e_all[...].reshape(PAIR, EMB), h) - twice(lq_b[...])
        s = jnp.where(twice(cid_b[...]) == y_row, -1e9, s)
        ex_ref[q] = s
        top = top_of(jnp.max(fold(s), axis=0))
        e = jnp.exp(ex_ref[q] - top)
        ex_ref[q] = e
        tot = sum_of(jnp.sum(fold(e), axis=0))
        rows = rows_f[part(q, TOK), :] + trow_o[part(q, TOK), :].astype(F32)
        tr_t[q] = rows.T
        z = sum_of((rows * h.astype(F32)).T)
        mine = (y_row >= first_row) & (y_row < first_row + CORES * ROWS)
        z_ref[row(q), :] = jnp.where(mine, z, 0.0)
        both = jnp.where(mine, jnp.maximum(top, z), top)
        tot = tot * jnp.exp(top - both) + jnp.where(mine, jnp.exp(jnp.where(mine, z - both, 0.0)), 0.0)
        mloc_ref[row(q), :] = top
        st_all[row(chip), 0, row(q), :] = both.reshape(1, 1, TOK)
        st_all[row(chip), 1, row(q), :] = tot.reshape(1, 1, TOK)

    stats_of(chip)
    for k in NEAR:
        h_got[k].wait_recv()
        stats_of(peers[k])
    st_got = spread(st_all, st_s, st_r, FAR)

    def tower_of(q):
        x = xs_all[q]
        xt_ref[:, part(q, TOK)] = x.T

        act = dot_nn(x, w_in_ref[...])
        tanh = tanh_of(act)
        cdf = 0.5 * (1.0 + tanh)
        slope = cdf + act * (0.5 * (1.0 - tanh * tanh)) * (ROOT_2_PI * (1.0 + 3.0 * CUBE * (act * act)))
        u_t = (act * cdf).astype(BF16).T
        for i in range(HID // LANES):
            tab_f[part(q * (HID // LANES) + i, TOK), :] = slope[:, i * LANES:(i + 1) * LANES]
        for r in halves:
            tab_b[part(q * 2 + r, HID), :] = u_t[:, r * HALF:(r + 1) * HALF]

    tower_of(chip)
    for k in NEAR[:3]:
        x_got[k].wait_recv()
        tower_of(peers[k])

    for k in NEAR:
        st_got[k].wait_recv()
    top_all = st_all[0, 0]
    for c in range(1, CHIPS):
        top_all = jnp.maximum(top_all, st_all[c, 0])
    tot_all = sum(st_all[c, 1] * jnp.exp(st_all[c, 0] - top_all) for c in range(CHIPS))
    log_norm = top_all + jnp.log(tot_all)
    l_ref[...] = log_norm
    f_ref[...] = jnp.exp(mloc_ref[...] - log_norm) * SHARE
    group = pl.ds(core * CHIPS, CHIPS)
    t_all = jnp.concatenate([tall[group, r, :] for r in halves], axis=1)
    mine_all = (t_all >= first_row) & (t_all < first_row + CORES * ROWS)
    z_all = z_ref[...]
    g_ref[...] = jnp.where(mine_all, (jnp.exp(jnp.where(mine_all, z_all - log_norm, 0.0)) - 1.0) * SHARE, 0.0)
    loss_all[row(me)] = (l_ref[row(chip), :] - sum_of(z_all)).reshape(1, 1, TOK)
    ls_got = to_all(loss_all, me, ls_s, ls_r, lambda device: device)

    def grads_of(q, is_first):
        h = hall[q]
        f_row = f_ref[row(q), :]

        p = (ex_ref[q] * f_row).astype(BF16)
        dh_acc[q] = dot_nn(e_t[...], p) + g_ref[row(q), :] * tr_t[q]
        de = dot_nn(p, h)
        de_acc[...] = de if is_first else de_acc[...] + de

    dh_got = arrivals(dh_in, dh_s, dh_r)
    for k in FAR:
        grads_of(peers[k], k == FAR[0])
        go(rcopy(dh_acc.at[peers[k]], dh_in.at[chip], dh_s.at[k], dh_r.at[chip], peers[k] * CORES + core))
    grads_of(chip, False)
    de_copy = swap(de_acc.at[part(oth, CAND), :], de_in, de_s, de_r)

    @pl.loop(0, CHIPS)
    def _(q):
        g_row = g_ref[row(q), :]
        for r in halves:
            col = column_of(g_row[:, r * HALF:(r + 1) * HALF])
            gh_ref[part((core * CHIPS + q) * 2 + r, HALF), :] = col * hall[q, r * HALF:(r + 1) * HALF, :].astype(F32)

    gh_copy = swap(gh_ref.at[part(core, GRP), :], gh_ref.at[part(core, GRP), :], gh_s, gh_r)

    for k in NEAR[3:]:
        x_got[k].wait_recv()
        tower_of(peers[k])

    de_copy.wait_recv()
    for r in range(CAND // KC):
        cand_f[r * KC:(r + 1) * KC, :] = de_acc[part(core * (CAND // KC) + r, KC), :] + de_in[r * KC:(r + 1) * KC, :]
    for c in ls_got:
        c.wait_recv()
    loss_out[...] = jnp.sum(jnp.sum(loss_all[...], axis=0), axis=1, keepdims=True) * SHARE
    gh_copy.wait_recv()
    outs = [
        pltpu.make_async_copy(gh_ref, gh_out, loc.at[0]),
        pltpu.make_async_copy(idx_vm, idx_out, loc.at[1]),
        pltpu.make_async_copy(bounds_vm, bounds_out, loc.at[2]),
        pltpu.make_async_copy(cand_f, gcand_out, loc.at[3]),
    ]
    for c in outs:
        c.start()

    for k in NEAR:
        dh_got[k].wait_recv()
    total = dh_acc[chip]
    for k in NEAR:
        total = total + dh_in[peers[k]]
    dhb_all[row(chip)] = total.T.astype(BF16).reshape(1, TOK, EMB)
    db_got = spread(dhb_all, db_s, db_r, FAR)

    def back_of(q):
        dh = dhb_all[q]

        e = dot_nt(dh, w_out_ref[...])
        slope = [tab_f[part(q * (HID // LANES) + i, TOK), :] for i in range(HID // LANES)]
        da_ref[part(q, TOK), :] = (jnp.concatenate(slope, axis=1) * e).astype(BF16)

    back_of(chip)
    for k in FAR:
        db_got[k].wait_recv()
        back_of(peers[k])

    w_got = []
    for i in range(HSTEPS):
        gwin[i] = dot_nn(xt_ref[...], da_ref[:, i * HB:(i + 1) * HB])
        w_got.append(swap(gwin.at[i], swin.at[i], wi_s.at[i], wi_r.at[i]))
    dh_flat = dhb_all[...].reshape(GRP, EMB)
    for i in range(HSTEPS):
        u_t = jnp.concatenate([tab_b[(q * 2 + r) * HID + i * HB:(q * 2 + r) * HID + (i + 1) * HB, :] for q in range(CHIPS) for r in halves], axis=1)
        gwout[i * HB:(i + 1) * HB, :] = dot_nn(u_t, dh_flat)
    w_got.append(swap(gwout, swout, wo_s, wo_r))
    for i in range(HSTEPS):
        w_got[i].wait_recv()
        w_got[i].wait_send()
        gwin[i] += swin[i]
        outs.append(pltpu.make_async_copy(gwin.at[i], dwin_out.at[:, part(i, HB)], loc.at[4 + i]))
        outs[-1].start()
    w_got[-1].wait_recv()
    w_got[-1].wait_send()
    gwout[...] += swout[...]
    outs.append(pltpu.make_async_copy(gwout, dwout_out, loc.at[4 + HSTEPS]))
    outs[-1].start()

    for c in sent:
        if not any(c is w for w in w_got):
            c.wait_send()
    for c in outs:
        c.wait()


def scatter_kernel(gcand_hbm, gh_hbm, idx_hbm, bounds_hbm, dwin_ref, dwout_ref, grad_out, dwin_out, dwout_out, acc, gcand, gh, idx_sm, bounds_sm, win_b, wout_b, sems):
    ins = [
        pltpu.make_async_copy(src, dst, sems.at[i])
        for i, (src, dst) in enumerate([(idx_hbm, idx_sm), (bounds_hbm, bounds_sm), (gcand_hbm, gcand), (gh_hbm, gh), (dwin_ref, win_b), (dwout_ref, wout_b)])
    ]
    for c in ins:
        c.start()

    @pl.loop(0, ROWS // KC)
    def _(i):
        acc[part(i, KC), :] = jnp.zeros((KC, EMB), F32)

    for c in ins[:3]:
        c.wait()

    @pl.loop(0, CAND // LANES)
    def _(i):
        for v in range(LANES):
            acc[row(idx_sm[DEVS + i // 2, i % 2, v]), :] = gcand[row(i * LANES + v), :]

    for c in ins[3:]:
        c.wait()
    outs = [pltpu.make_async_copy(win_b, dwin_out, sems.at[6]), pltpu.make_async_copy(wout_b, dwout_out, sems.at[7])]
    for c in outs:
        c.start()

    @pl.loop(0, DEVS)
    def _(s):
        def add(i, carry):
            for v in range(CROW):
                r = idx_sm[s, i >> 4, (i & 15) * CROW + v]
                acc[row(r), :] += gh[row(s * TOK + i * CROW + v), :]
            return carry

        lax.fori_loop(bounds_sm[s, 0, 0] >> 3, (bounds_sm[s, 0, 1] + 7) >> 3, add, 0)

    outs.append(pltpu.make_async_copy(acc.at[pl.ds(0, ROWS), :], grad_out, sems.at[8]))
    outs[-1].start()
    for c in outs:
        c.wait()


def solution(mesh):
    def local_step(features, w_in, w_out, table_blk, cand_ids, log_q, targets):
        vmem = pl.BlockSpec(memory_space=pltpu.VMEM)
        hbm = pl.BlockSpec(memory_space=pl.ANY)
        dma = pltpu.SemaphoreType.DMA
        sds = jax.ShapeDtypeStruct

        def v(dtype, *shape):
            return pltpu.VMEM(shape, dtype)

        chips = dma((CHIPS,))
        idx_shape = (DEVS + CROW // 2, 2, LANES)
        loss, gcand, gh, idx, bounds, dwin, dwout = pl.pallas_call(
            main_kernel,
            name="main_kernel",
            out_shape=(
                sds((1, 1), F32), sds((CAND, EMB), F32), sds((TOTAL, EMB), F32),
                sds(idx_shape, I32), sds((DEVS, 1, LANES), I32), sds((IN, HID), F32), sds((HID, EMB), F32),
            ),
            in_specs=[vmem] * 4 + [hbm] * 3,
            out_specs=(vmem,) + (hbm,) * 6,
            scratch_shapes=[
                v(BF16, ROWS, EMB),
                v(F32, ROWS + CROW, EMB),
                v(I32, DEVS, 2, LANES),
                v(I32, *idx_shape),
                pltpu.SMEM(idx_shape, I32),
                v(I32, CORES, CROW, LANES),
                v(F32, CORES, CROW, LANES),
                v(BF16, CHIPS, TOK, IN),
                v(BF16, IN, GRP),
                v(BF16, TOK, HID),
                v(BF16, CHIPS, TOK, EMB),
                v(F32, GRP, EMB),
                v(F32, CAND, EMB),
                v(BF16, CORES, CAND, EMB),
                v(BF16, EMB, PAIR),
                v(I32, PAIR, LANES),
                v(F32, PAIR, LANES),
                v(BF16, GRP, EMB),
                v(BF16, GRP, EMB),
                v(F32, CHIPS, EMB, TOK),
                v(F32, CHIPS, PAIR, TOK),
                v(F32, CHIPS, 2, CHIPS, TOK),
                v(F32, CHIPS, TOK),
                v(F32, CHIPS, TOK),
                v(F32, CHIPS, TOK),
                v(F32, CHIPS, TOK),
                v(F32, CHIPS, TOK),
                v(F32, TOTAL, EMB),
                v(F32, CHIPS, EMB, TOK),
                v(F32, CHIPS, EMB, TOK),
                v(BF16, CHIPS, TOK, EMB),
                v(BF16, GRP, HID),
                v(F32, PAIR, EMB),
                v(F32, CAND, EMB),
                v(F32, HSTEPS, IN, HB),
                v(F32, HID, EMB),
                v(F32, HSTEPS, IN, HB),
                v(F32, HID, EMB),
                v(F32, DEVS, 1, TOK),
                v(I32, DEVS, 1, LANES),
                dma((DEVS - 1,)), dma((DEVS,)),
                chips, chips,
                chips, chips,
                dma, dma,
                dma, dma,
                chips, chips,
                chips, chips,
                dma, dma,
                dma, dma,
                chips, chips,
                dma((HSTEPS,)), dma((HSTEPS,)),
                dma, dma,
                dma((DEVS - 1,)), dma((DEVS,)),
                dma((CROW + HSTEPS,)),
            ],
            compiler_params=pltpu.CompilerParams(collective_id=0, has_side_effects=True, vmem_limit_bytes=VMEM_LIMIT),
        )(features, w_in, w_out, targets.reshape(2, LANES), cand_ids.reshape(DEVS, CROW, LANES), log_q.reshape(DEVS, CROW, LANES), table_blk)
        grad_blk, grad_in, grad_out = pl.pallas_call(
            scatter_kernel,
            name="scatter_kernel",
            out_shape=(sds((ROWS, EMB), F32), sds((IN, HID), F32), sds((HID, EMB), F32)),
            in_specs=[hbm] * 6,
            out_specs=(hbm,) * 3,
            scratch_shapes=[
                v(F32, ROWS + CROW, EMB),
                v(F32, CAND, EMB),
                v(F32, TOTAL, EMB),
                pltpu.SMEM(idx_shape, I32),
                pltpu.SMEM((DEVS, 1, LANES), I32),
                v(F32, IN, HID),
                v(F32, HID, EMB),
                dma((9,)),
            ],
            compiler_params=pltpu.CompilerParams(vmem_limit_bytes=VMEM_LIMIT),
        )(gcand, gh, idx, bounds, dwin, dwout)
        return loss[0, 0], grad_blk, grad_in, grad_out

    return jax.shard_map(local_step, mesh=mesh, in_specs=(P("dp", None), P(), P(), P("dp", None), P(), P(), P("dp")), out_specs=(P(), P("dp", None), P(), P()), check_vma=False)
```

```python
import jax
import jax.numpy as jnp
from jax import lax
from jax.experimental import pallas as pl
from jax.experimental.pallas import tpu as pltpu
from jax.sharding import PartitionSpec as P

F32 = jnp.float32
BF16 = jnp.bfloat16
I32 = jnp.int32
MESH = pl.DeviceIdType.MESH

CORES = 2
CHIPS = 8
DEVS = 16
LANES = 128
TOK = 256
HALF = 128
GRP = 2048
CAND = 1024
PAIR = 2048
CROW = 8
EMB = 128
HID = 1024
IN = 256
ROWS = 16384
TOTAL = 4096
KC = 256
HB = 256
HSTEPS = HID // HB
ROOT_2_PI = 0.7978845608028654
CUBE = 0.044715
SHARE = 1.0 / TOTAL
VMEM_LIMIT = 64 * 1024 * 1024 - 65536

NEAR = (1, 2, 4, 3, 5, 6, 7)
FAR = (7, 6, 5, 3, 4, 2, 1)


def dot_nt(lhs, rhs):
    return lax.dot_general(lhs, rhs, (((1,), (1,)), ((), ())), preferred_element_type=F32)


def dot_nn(lhs, rhs):
    return jnp.dot(lhs, rhs, preferred_element_type=F32)


def column_of(row):
    return jnp.broadcast_to(row, (LANES, LANES)).T


def top_of(x):
    return jnp.max(x, axis=0, keepdims=True)


def sum_of(x):
    return jnp.sum(x, axis=0, keepdims=True)


def part(i, size):
    return pl.ds(pl.multiple_of(i * size, size), size)


def row(i):
    return pl.ds(i, 1)


def tanh_of(act):
    return jnp.tanh(ROOT_2_PI * (act + CUBE * (act * act * act)))


def main_kernel(
    x_hbm, w_in_hbm, w_out_hbm, tgt_hbm, cand_hbm, logq_hbm, table_hbm,
    loss_out, gcand_out, gh_out, idx_out, bounds_out, dwin_out, dwout_out,
    x_ref, w_in_ref, w_out_ref, tgt_ref, tab_b, tab_f, tall, idx_vm, idx_sm, cand_vm, logq_vm, xs_all, xt_ref, u_ref, hall,
    rows_f, cand_f, e_all, e_t, cid_b, lq_b, trow_s, trow_o, tr_t,
    ex_ref, st_all, mloc_ref, z_ref, l_ref, f_ref, g_ref, gh_ref,
    dh_acc, dh_in, dhb_all, da_ref, de_acc, de_in, gwin, gwout, swin, swout, loss_all, bounds_vm,
    tgt_s, tgt_r, h_s, h_r, x_s, x_r, e_s, e_r, tr_s, tr_r, st_s, st_r, dh_s, dh_r, de_s, de_r, gh_s, gh_r,
    db_s, db_r, wi_s, wi_r, wo_s, wo_r, ls_s, ls_r, loc,
):
    me = lax.axis_index("dp")
    chip = me // CORES
    core = me % CORES
    oth = 1 - core
    sib = chip * CORES + oth
    base = me * ROWS
    zc = chip // (CHIPS // 2)
    first_row = chip * (CORES * ROWS)

    def flip(k):
        out = 0
        for bit in (1, 2, 4):
            out = out + (((chip // bit) + (k // bit)) % 2) * bit
        return out

    peers = {k: flip(k) for k in NEAR}

    def slot_of(device):
        return (device % CORES) * CHIPS + device // CORES

    def rcopy(src, dst, ssem, rsem, dev):
        return pltpu.make_async_remote_copy(src_ref=src, dst_ref=dst, send_sem=ssem, recv_sem=rsem, device_id=(dev,), device_id_type=MESH)

    sent = []

    def go(copy):
        copy.start()
        sent.append(copy)
        return copy

    def swap(src, dst, ssem, rsem):
        return go(rcopy(src, dst, ssem, rsem, sib))

    def arrivals(ref, ssem, rsem):
        return {k: rcopy(ref.at[src], ref.at[src], ssem.at[k], rsem.at[src], src * CORES + core) for k, src in peers.items()}

    def spread(ref, ssem, rsem, ks):
        got = arrivals(ref, ssem, rsem)
        for k in ks:
            go(rcopy(ref.at[chip], ref.at[chip], ssem.at[k], rsem.at[chip], peers[k] * CORES + core))
        return got

    def to_all(ref, slot, ssem, rsem, slots):
        got = []
        for i in range(DEVS - 1):
            src = slots(lax.rem(me + (DEVS - 1) - i, DEVS))
            got.append(rcopy(ref.at[src], ref.at[src], ssem.at[i], rsem.at[src], others[i]))
        for i, dev in enumerate(others):
            go(rcopy(ref.at[slot], ref.at[slot], ssem.at[i], rsem.at[slot], dev))
        return got

    others = [lax.rem(me + k, DEVS) for k in range(1, DEVS)]

    barrier = pltpu.get_barrier_semaphore()
    for dev in others:
        pl.semaphore_signal(barrier, inc=1, device_id=(dev,), device_id_type=MESH)

    chip_blocks = pl.ds(chip * CORES, CORES)
    inputs = [(tgt_hbm, tgt_ref), (x_hbm, x_ref), (w_in_hbm, w_in_ref), (w_out_hbm, w_out_ref)]
    inputs = [pltpu.make_async_copy(src, dst, loc.at[3 + i]) for i, (src, dst) in enumerate(inputs)]
    for c in inputs:
        c.start()
    early = [
        pltpu.make_async_copy(cand_hbm.at[chip_blocks], cand_vm, loc.at[0]),
        pltpu.make_async_copy(logq_hbm.at[chip_blocks], logq_vm, loc.at[1]),
        pltpu.make_async_copy(table_hbm, tab_b, loc.at[2]),
    ]
    for c in early:
        c.start()
    inputs[0].wait()

    lane = lax.broadcasted_iota(I32, (1, LANES), 1)
    halves = range(TOK // HALF)
    tgt = [tgt_ref[q:q + 1, :] for q in halves]
    key = [tgt[q] * TOK + (lane + q * HALF) for q in halves]
    key_col = [column_of(k) for k in key]
    sub = lax.broadcasted_iota(I32, (TOK, LANES), 0)
    hot = [sub == sum(sum_of((key_col[r] < key[q]).astype(I32)) for r in halves) for q in halves]
    perm = jnp.concatenate([jnp.where(h, 1.0, 0.0).astype(BF16) for h in hot], axis=1)
    moved = [jnp.where(hot[q], jnp.broadcast_to(tgt[q].astype(F32), (TOK, LANES)), 0.0) for q in halves]
    my_slot = core * CHIPS + chip
    for r in halves:
        line = sum(sum_of(m[r * HALF:(r + 1) * HALF, :].T) for m in moved)
        tall[row(my_slot), row(r), :] = line.astype(I32).reshape(1, 1, LANES)

    for c in inputs[1:]:
        c.wait()
    xs = dot_nn(perm, x_ref[...]).astype(BF16)
    xs_all[row(chip)] = xs.reshape(1, TOK, IN)
    act = dot_nn(xs, w_in_ref[...])
    u_ref[...] = (act * (0.5 * (1.0 + tanh_of(act)))).astype(BF16)
    hall[row(chip)] = dot_nn(u_ref[...], w_out_ref[...]).astype(BF16).reshape(1, TOK, EMB)

    pl.semaphore_wait(barrier, DEVS - 1)
    tgt_got = to_all(tall, my_slot, tgt_s, tgt_r, slot_of)
    h_got = spread(hall, h_s, h_r, NEAR)
    x_got = spread(xs_all, x_s, x_r, NEAR)

    for c in early:
        c.wait()
    for r in range(CROW):
        idx_vm[DEVS + r // 2, r % 2:r % 2 + 1, :] = jnp.clip(cand_vm[core, r:r + 1, :] - base, 0, ROWS - 1)
    cand_at = pl.ds(DEVS, CROW // 2)
    cand_copy = pltpu.make_async_copy(idx_vm.at[cand_at], idx_sm.at[cand_at], loc.at[0])
    cand_copy.start()

    @pl.loop(0, ROWS // KC)
    def _(i):
        tab_f[part(i, KC), :] = tab_b[part(i, KC), :].astype(F32)

    tab_f[pl.ds(ROWS, CROW), :] = jnp.zeros((CROW, EMB), F32)
    cand_copy.wait()

    def gather_rows(slot, dst, first):
        for v in range(TOK):
            dst[row(first + v), :] = tab_f[row(idx_sm[slot, v // LANES, v % LANES]), :]

    @pl.loop(0, CAND // TOK)
    def _(i):
        gather_rows(DEVS + i, cand_f, i * TOK)

    e_all[row(core)] = cand_f[...].astype(BF16).reshape(1, CAND, EMB)
    e_copy = swap(e_all.at[core], e_all.at[core], e_s, e_r)

    for c in tgt_got:
        c.wait_recv()
    loc_idx = tall[...] - base
    own = (loc_idx >= 0) & (loc_idx < ROWS)
    idx_vm[0:DEVS] = jnp.where(own, loc_idx, ROWS)

    def count(mask):
        return jnp.sum(jnp.sum(mask.astype(F32), axis=2, keepdims=True), axis=1, keepdims=True)

    lane3 = lax.broadcasted_iota(I32, (DEVS, 1, LANES), 2)
    bounds_vm[...] = jnp.where(lane3 == 0, count(loc_idx < 0), count(loc_idx < ROWS)).astype(I32)
    tok_at = pl.ds(0, DEVS)
    idx_copy = pltpu.make_async_copy(idx_vm.at[tok_at], idx_sm.at[tok_at], loc.at[0])
    idx_copy.start()
    idx_copy.wait()

    @pl.loop(0, CHIPS)
    def _(q):
        gather_rows(oth * CHIPS + q, rows_f, q * TOK)

    trow_s[...] = rows_f[...].astype(BF16)
    tr_copy = swap(trow_s, trow_o, tr_s, tr_r)

    @pl.loop(0, CHIPS)
    def _(q):
        gather_rows(core * CHIPS + q, rows_f, q * TOK)

    for b in range(CORES):
        for r in range(CROW):
            at = b * CAND + r * LANES
            cid_b[at:at + LANES, :] = column_of(cand_vm[b, r:r + 1, :])
            lq_b[at:at + LANES, :] = column_of(logq_vm[b, r:r + 1, :])
    e_copy.wait_recv()
    tr_copy.wait_recv()

    def twice(x):
        return jnp.concatenate([x, x], axis=1)

    def fold(x):
        return x.reshape(PAIR // 8, 8, TOK)

    def stats_of(q):
        h = hall[q]
        ids = tall[core * CHIPS + q]
        y_row = jnp.concatenate([ids[r:r + 1, :] for r in halves], axis=1)

        s = dot_nt(e_all[...].reshape(PAIR, EMB), h) - twice(lq_b[...])
        s = jnp.where(twice(cid_b[...]) == y_row, -1e9, s)
        ex_ref[q] = s
        top = top_of(jnp.max(fold(s), axis=0))
        e = jnp.exp(ex_ref[q] - top)
        ex_ref[q] = e
        tot = sum_of(jnp.sum(fold(e), axis=0))
        rows = rows_f[part(q, TOK), :] + trow_o[part(q, TOK), :].astype(F32)
        tr_t[q] = rows.T
        z = sum_of((rows * h.astype(F32)).T)
        mine = (y_row >= first_row) & (y_row < first_row + CORES * ROWS)
        z_ref[row(q), :] = jnp.where(mine, z, 0.0)
        both = jnp.where(mine, jnp.maximum(top, z), top)
        tot = tot * jnp.exp(top - both) + jnp.where(mine, jnp.exp(jnp.where(mine, z - both, 0.0)), 0.0)
        mloc_ref[row(q), :] = top
        st_all[row(chip), 0, row(q), :] = both.reshape(1, 1, TOK)
        st_all[row(chip), 1, row(q), :] = tot.reshape(1, 1, TOK)

    stats_of(chip)
    for k in NEAR:
        h_got[k].wait_recv()
        stats_of(peers[k])
    st_got = spread(st_all, st_s, st_r, FAR)

    def tower_of(q):
        x = xs_all[q]
        xt_ref[:, part(q, TOK)] = x.T

        act = dot_nn(x, w_in_ref[...])
        tanh = tanh_of(act)
        cdf = 0.5 * (1.0 + tanh)
        slope = cdf + act * (0.5 * (1.0 - tanh * tanh)) * (ROOT_2_PI * (1.0 + 3.0 * CUBE * (act * act)))
        u_t = (act * cdf).astype(BF16).T
        for i in range(HID // LANES):
            tab_f[part(q * (HID // LANES) + i, TOK), :] = slope[:, i * LANES:(i + 1) * LANES]
        for r in halves:
            tab_b[part(q * 2 + r, HID), :] = u_t[:, r * HALF:(r + 1) * HALF]

    for b in range(CORES):
        e_t[:, b * CAND:(b + 1) * CAND] = e_all[b].T
    tower_of(chip)
    for k in NEAR[:3]:
        x_got[k].wait_recv()
        tower_of(peers[k])

    for k in NEAR:
        st_got[k].wait_recv()
    top_all = st_all[0, 0]
    for c in range(1, CHIPS):
        top_all = jnp.maximum(top_all, st_all[c, 0])
    tot_all = sum(st_all[c, 1] * jnp.exp(st_all[c, 0] - top_all) for c in range(CHIPS))
    log_norm = top_all + jnp.log(tot_all)
    l_ref[...] = log_norm
    f_ref[...] = jnp.exp(mloc_ref[...] - log_norm) * SHARE
    group = pl.ds(core * CHIPS, CHIPS)
    t_all = jnp.concatenate([tall[group, r, :] for r in halves], axis=1)
    mine_all = (t_all >= first_row) & (t_all < first_row + CORES * ROWS)
    z_all = z_ref[...]
    g_ref[...] = jnp.where(mine_all, (jnp.exp(jnp.where(mine_all, z_all - log_norm, 0.0)) - 1.0) * SHARE, 0.0)
    loss_all[row(me)] = (l_ref[row(chip), :] - sum_of(z_all)).reshape(1, 1, TOK)
    ls_got = to_all(loss_all, me, ls_s, ls_r, lambda device: device)

    def grads_of(q, is_first):
        h = hall[q]
        f_row = f_ref[row(q), :]

        p = (ex_ref[q] * f_row).astype(BF16)
        dh_acc[q] = dot_nn(e_t[...], p) + g_ref[row(q), :] * tr_t[q]
        de = dot_nn(p, h)
        de_acc[...] = de if is_first else de_acc[...] + de

    parts = [pl.ds(r * (EMB // 2), EMB // 2) for r in range(2)]
    JOIN = {7: (1, 6), 6: (2, 4), 5: (4, 1), 3: (1, 2), 4: (4, 0), 1: (1, 0), 2: (2, 0)}

    def pass_on(k, r):
        link = JOIN[k][0]
        go(rcopy(dh_acc.at[peers[k], parts[r], :], dh_in.at[k, parts[r], :], dh_s.at[r, k], dh_r.at[r, k], peers[link] * CORES + core))

    def join(k, r):
        link, into = JOIN[k]
        rcopy(dh_in.at[k, parts[r], :], dh_in.at[k, parts[r], :], dh_s.at[r, k], dh_r.at[r, k], peers[link] * CORES + core).wait_recv()
        place = peers[into] if into else chip
        dh_acc[place, parts[r], :] += dh_in[k, parts[r], :]

    def relay(k, r):
        join(k, r)
        pass_on(JOIN[k][1], r)

    for k in (7, 6, 3, 5, 4):
        grads_of(peers[k], k == FAR[0])
        if k in (7, 3, 5):
            pass_on(k, 0)
            pass_on(k, 1)
    relay(7, 0)
    grads_of(peers[1], False)
    grads_of(peers[2], False)
    relay(7, 1)
    for r in range(2):
        for k in (5, 3, 6):
            relay(k, r)
    grads_of(chip, False)
    de_copy = swap(de_acc.at[part(oth, CAND), :], de_in, de_s, de_r)

    @pl.loop(0, CHIPS)
    def _(q):
        g_row = g_ref[row(q), :]
        for r in halves:
            col = column_of(g_row[:, r * HALF:(r + 1) * HALF])
            gh_ref[part((core * CHIPS + q) * 2 + r, HALF), :] = col * hall[q, r * HALF:(r + 1) * HALF, :].astype(F32)

    gh_copy = swap(gh_ref.at[part(core, GRP), :], gh_ref.at[part(core, GRP), :], gh_s, gh_r)

    for k in NEAR[3:]:
        x_got[k].wait_recv()
        tower_of(peers[k])

    de_copy.wait_recv()
    for r in range(CAND // KC):
        cand_f[r * KC:(r + 1) * KC, :] = de_acc[part(core * (CAND // KC) + r, KC), :] + de_in[r * KC:(r + 1) * KC, :]
    for c in ls_got:
        c.wait_recv()
    loss_out[...] = jnp.sum(jnp.sum(loss_all[...], axis=0), axis=1, keepdims=True) * SHARE
    gh_copy.wait_recv()
    outs = [
        pltpu.make_async_copy(gh_ref, gh_out, loc.at[0]),
        pltpu.make_async_copy(idx_vm, idx_out, loc.at[1]),
        pltpu.make_async_copy(bounds_vm, bounds_out, loc.at[2]),
        pltpu.make_async_copy(cand_f, gcand_out, loc.at[3]),
    ]
    for c in outs:
        c.start()

    for k in (2, 1, 4):
        for r in range(2):
            join(k, r)
    total = dh_acc[chip]
    dhb_all[row(chip)] = total.T.astype(BF16).reshape(1, TOK, EMB)
    db_got = spread(dhb_all, db_s, db_r, (7, 6, 5, 4, 3, 2, 1))

    def back_of(q):
        dh = dhb_all[q]

        e = dot_nt(dh, w_out_ref[...])
        slope = [tab_f[part(q * (HID // LANES) + i, TOK), :] for i in range(HID // LANES)]
        da_ref[part(q, TOK), :] = (jnp.concatenate(slope, axis=1) * e).astype(BF16)

    w_got = []
    for half, ks in enumerate(((7, 6, 5, 4), (3, 2, 1, 0))):
        for k in ks:
            if k:
                db_got[k].wait_recv()
            back_of(peers[k] if k else chip)
        z_side = zc if half else 1 - zc
        xt = xt_ref[:, part(z_side, GRP // 2)]
        for i in range(HSTEPS):
            new = dot_nn(xt, da_ref[part(z_side, GRP // 2), i * HB:(i + 1) * HB])
            gwin[i] = gwin[i] + new if half else new
            if half:
                w_got.append(swap(gwin.at[i], swin.at[i], wi_s.at[i], wi_r.at[i]))
        near = CHIPS // 2
        dh_flat = dhb_all[pl.ds(z_side * near, near)].reshape(GRP // 2, EMB)
        for i in range(HSTEPS):
            at = [((z_side * near + q) * 2 + r) * HID + i * HB for q in range(near) for r in halves]
            u_t = jnp.concatenate([tab_b[pl.ds(pl.multiple_of(a, HB), HB), :] for a in at], axis=1)
            new = dot_nn(u_t, dh_flat)
            here = gwout.at[i * HB:(i + 1) * HB, :]
            here[...] = here[...] + new if half else new
    w_got.append(swap(gwout, swout, wo_s, wo_r))
    for i in range(HSTEPS):
        w_got[i].wait_recv()
        w_got[i].wait_send()
        gwin[i] += swin[i]
        outs.append(pltpu.make_async_copy(gwin.at[i], dwin_out.at[:, part(i, HB)], loc.at[4 + i]))
        outs[-1].start()
    w_got[-1].wait_recv()
    w_got[-1].wait_send()
    gwout[...] += swout[...]
    outs.append(pltpu.make_async_copy(gwout, dwout_out, loc.at[4 + HSTEPS]))
    outs[-1].start()

    for c in sent:
        if not any(c is w for w in w_got):
            c.wait_send()
    for c in outs:
        c.wait()


def scatter_kernel(gcand_hbm, gh_hbm, idx_hbm, bounds_hbm, dwin_ref, dwout_ref, grad_out, dwin_out, dwout_out, acc, gcand, gh, idx_sm, bounds_sm, win_b, wout_b, sems):
    ins = [
        pltpu.make_async_copy(src, dst, sems.at[i])
        for i, (src, dst) in enumerate([(idx_hbm, idx_sm), (bounds_hbm, bounds_sm), (gcand_hbm, gcand), (gh_hbm, gh), (dwin_ref, win_b), (dwout_ref, wout_b)])
    ]
    for c in ins:
        c.start()

    @pl.loop(0, ROWS // KC)
    def _(i):
        acc[part(i, KC), :] = jnp.zeros((KC, EMB), F32)

    for c in ins[:3]:
        c.wait()

    @pl.loop(0, CAND // LANES)
    def _(i):
        for v in range(LANES):
            acc[row(idx_sm[DEVS + i // 2, i % 2, v]), :] = gcand[row(i * LANES + v), :]

    for c in ins[3:]:
        c.wait()
    outs = [pltpu.make_async_copy(win_b, dwin_out, sems.at[6]), pltpu.make_async_copy(wout_b, dwout_out, sems.at[7])]
    for c in outs:
        c.start()

    @pl.loop(0, DEVS)
    def _(s):
        def add(i, carry):
            for v in range(CROW):
                r = idx_sm[s, i >> 4, (i & 15) * CROW + v]
                acc[row(r), :] += gh[row(s * TOK + i * CROW + v), :]
            return carry

        lax.fori_loop(bounds_sm[s, 0, 0] >> 3, (bounds_sm[s, 0, 1] + 7) >> 3, add, 0)

    outs.append(pltpu.make_async_copy(acc.at[pl.ds(0, ROWS), :], grad_out, sems.at[8]))
    outs[-1].start()
    for c in outs:
        c.wait()


def solution(mesh):
    def local_step(features, w_in, w_out, table_blk, cand_ids, log_q, targets):
        vmem = pl.BlockSpec(memory_space=pltpu.VMEM)
        hbm = pl.BlockSpec(memory_space=pl.ANY)
        dma = pltpu.SemaphoreType.DMA
        sds = jax.ShapeDtypeStruct

        def v(dtype, *shape):
            return pltpu.VMEM(shape, dtype)

        chips = dma((CHIPS,))
        idx_shape = (DEVS + CROW // 2, 2, LANES)
        loss, gcand, gh, idx, bounds, dwin, dwout = pl.pallas_call(
            main_kernel,
            name="main_kernel",
            out_shape=(
                sds((1, 1), F32), sds((CAND, EMB), F32), sds((TOTAL, EMB), F32),
                sds(idx_shape, I32), sds((DEVS, 1, LANES), I32), sds((IN, HID), F32), sds((HID, EMB), F32),
            ),
            in_specs=[hbm] * 7,
            out_specs=(vmem,) + (hbm,) * 6,
            scratch_shapes=[
                v(BF16, TOK, IN),
                v(BF16, IN, HID),
                v(BF16, HID, EMB),
                v(I32, 2, LANES),
                v(BF16, ROWS, EMB),
                v(F32, ROWS + CROW, EMB),
                v(I32, DEVS, 2, LANES),
                v(I32, *idx_shape),
                pltpu.SMEM(idx_shape, I32),
                v(I32, CORES, CROW, LANES),
                v(F32, CORES, CROW, LANES),
                v(BF16, CHIPS, TOK, IN),
                v(BF16, IN, GRP),
                v(BF16, TOK, HID),
                v(BF16, CHIPS, TOK, EMB),
                v(F32, GRP, EMB),
                v(F32, CAND, EMB),
                v(BF16, CORES, CAND, EMB),
                v(BF16, EMB, PAIR),
                v(I32, PAIR, LANES),
                v(F32, PAIR, LANES),
                v(BF16, GRP, EMB),
                v(BF16, GRP, EMB),
                v(F32, CHIPS, EMB, TOK),
                v(F32, CHIPS, PAIR, TOK),
                v(F32, CHIPS, 2, CHIPS, TOK),
                v(F32, CHIPS, TOK),
                v(F32, CHIPS, TOK),
                v(F32, CHIPS, TOK),
                v(F32, CHIPS, TOK),
                v(F32, CHIPS, TOK),
                v(F32, TOTAL, EMB),
                v(F32, CHIPS, EMB, TOK),
                v(F32, CHIPS, EMB, TOK),
                v(BF16, CHIPS, TOK, EMB),
                v(BF16, GRP, HID),
                v(F32, PAIR, EMB),
                v(F32, CAND, EMB),
                v(F32, HSTEPS, IN, HB),
                v(F32, HID, EMB),
                v(F32, HSTEPS, IN, HB),
                v(F32, HID, EMB),
                v(F32, DEVS, 1, TOK),
                v(I32, DEVS, 1, LANES),
                dma((DEVS - 1,)), dma((DEVS,)),
                chips, chips,
                chips, chips,
                dma, dma,
                dma, dma,
                chips, chips,
                dma((2, CHIPS)), dma((2, CHIPS)),
                dma, dma,
                dma, dma,
                chips, chips,
                dma((HSTEPS,)), dma((HSTEPS,)),
                dma, dma,
                dma((DEVS - 1,)), dma((DEVS,)),
                dma((CROW + HSTEPS,)),
            ],
            compiler_params=pltpu.CompilerParams(collective_id=0, has_side_effects=True, vmem_limit_bytes=VMEM_LIMIT),
        )(features, w_in, w_out, targets.reshape(2, LANES), cand_ids.reshape(DEVS, CROW, LANES), log_q.reshape(DEVS, CROW, LANES), table_blk)
        grad_blk, grad_in, grad_out = pl.pallas_call(
            scatter_kernel,
            name="scatter_kernel",
            out_shape=(sds((ROWS, EMB), F32), sds((IN, HID), F32), sds((HID, EMB), F32)),
            in_specs=[hbm] * 6,
            out_specs=(hbm,) * 3,
            scratch_shapes=[
                v(F32, ROWS + CROW, EMB),
                v(F32, CAND, EMB),
                v(F32, TOTAL, EMB),
                pltpu.SMEM(idx_shape, I32),
                pltpu.SMEM((DEVS, 1, LANES), I32),
                v(F32, IN, HID),
                v(F32, HID, EMB),
                dma((9,)),
            ],
            compiler_params=pltpu.CompilerParams(vmem_limit_bytes=VMEM_LIMIT),
        )(gcand, gh, idx, bounds, dwin, dwout)
        return loss[0, 0], grad_blk, grad_in, grad_out

    return jax.shard_map(local_step, mesh=mesh, in_specs=(P("dp", None), P(), P(), P("dp", None), P(), P(), P("dp")), out_specs=(P(), P("dp", None), P(), P()), check_vma=False)
```

```python
import jax
import jax.numpy as jnp
from jax import lax
from jax.experimental import pallas as pl
from jax.experimental.pallas import tpu as pltpu
from jax.sharding import PartitionSpec as P

F32 = jnp.float32
BF16 = jnp.bfloat16
I32 = jnp.int32
MESH = pl.DeviceIdType.MESH

CORES = 2
CHIPS = 8
DEVS = 16
LANES = 128
TOK = 256
HALF = 128
GRP = 2048
CAND = 1024
PAIR = 2048
CROW = 8
EMB = 128
HID = 1024
IN = 256
ROWS = 16384
TOTAL = 4096
KC = 256
HB = 256
HSTEPS = HID // HB
ROOT_2_PI = 0.7978845608028654
CUBE = 0.044715
SHARE = 1.0 / TOTAL
VMEM_LIMIT = 64 * 1024 * 1024 - 65536

NEAR = (1, 2, 4, 3, 5, 6, 7)
FAR = (7, 6, 5, 3, 4, 2, 1)
DOWN = (7, 6, 5, 4, 3, 2, 1)
TOWERS = (3, 5, 6, 7, 4, 2, 1)


def dot_nt(lhs, rhs):
    return lax.dot_general(lhs, rhs, (((1,), (1,)), ((), ())), preferred_element_type=F32)


def dot_nn(lhs, rhs):
    return jnp.dot(lhs, rhs, preferred_element_type=F32)


def column_of(row):
    return jnp.broadcast_to(row, (LANES, LANES)).T


def top_of(x):
    return jnp.max(x, axis=0, keepdims=True)


def sum_of(x):
    return jnp.sum(x, axis=0, keepdims=True)


def part(i, size):
    return pl.ds(pl.multiple_of(i * size, size), size)


def row(i):
    return pl.ds(i, 1)


def tanh_of(act):
    return jnp.tanh(ROOT_2_PI * (act + CUBE * (act * act * act)))


def main_kernel(
    x_hbm, w_in_hbm, w_out_hbm, tgt_hbm, cand_hbm, logq_hbm, table_hbm,
    loss_out, gcand_out, gh_out, idx_out, bounds_out, dwin_out, dwout_out,
    x_ref, w_in_ref, w_out_ref, tgt_ref, tab_b, tab_f, tall, idx_vm, idx_sm, cand_vm, logq_vm, xs_all, xt_ref, u_ref, hall,
    rows_f, cand_f, e_all, e_t, cid_b, lq_b, trow_s, trow_o, tr_t,
    ex_ref, st_all, mloc_ref, z_ref, l_ref, f_ref, g_ref, gh_ref,
    dh_acc, dh_in, dhb_all, da_ref, de_acc, de_in, gwin, gwout, swin, swout, loss_all, bounds_vm,
    tgt_s, tgt_r, h_s, h_r, x_s, x_r, e_s, e_r, tr_s, tr_r, st_s, st_r, dh_s, dh_r, de_s, de_r, gh_s, gh_r,
    db_s, db_r, wi_s, wi_r, wo_s, wo_r, ls_s, ls_r, loc,
):
    me = lax.axis_index("dp")
    chip = me // CORES
    core = me % CORES
    oth = 1 - core
    sib = chip * CORES + oth
    base = me * ROWS
    zc = chip // (CHIPS // 2)
    first_row = chip * (CORES * ROWS)

    def flip(k):
        out = 0
        for bit in (1, 2, 4):
            out = out + (((chip // bit) + (k // bit)) % 2) * bit
        return out

    peers = {k: flip(k) for k in NEAR}

    def slot_of(device):
        return (device % CORES) * CHIPS + device // CORES

    def rcopy(src, dst, ssem, rsem, dev):
        return pltpu.make_async_remote_copy(src_ref=src, dst_ref=dst, send_sem=ssem, recv_sem=rsem, device_id=(dev,), device_id_type=MESH)

    sent = []

    def go(copy):
        copy.start()
        sent.append(copy)
        return copy

    def swap(src, dst, ssem, rsem):
        return go(rcopy(src, dst, ssem, rsem, sib))

    def arrivals(ref, ssem, rsem):
        return {k: rcopy(ref.at[src], ref.at[src], ssem.at[k], rsem.at[src], src * CORES + core) for k, src in peers.items()}

    def spread(ref, ssem, rsem, ks):
        got = arrivals(ref, ssem, rsem)
        for k in ks:
            go(rcopy(ref.at[chip], ref.at[chip], ssem.at[k], rsem.at[chip], peers[k] * CORES + core))
        return got

    def to_all(ref, slot, ssem, rsem, slots):
        got = []
        for i in range(DEVS - 1):
            src = slots(lax.rem(me + (DEVS - 1) - i, DEVS))
            got.append(rcopy(ref.at[src], ref.at[src], ssem.at[i], rsem.at[src], others[i]))
        for i, dev in enumerate(others):
            go(rcopy(ref.at[slot], ref.at[slot], ssem.at[i], rsem.at[slot], dev))
        return got

    others = [lax.rem(me + k, DEVS) for k in range(1, DEVS)]

    barrier = pltpu.get_barrier_semaphore()
    for dev in others:
        pl.semaphore_signal(barrier, inc=1, device_id=(dev,), device_id_type=MESH)

    chip_blocks = pl.ds(chip * CORES, CORES)
    inputs = [(tgt_hbm, tgt_ref), (x_hbm, x_ref), (w_in_hbm, w_in_ref), (w_out_hbm, w_out_ref)]
    inputs = [pltpu.make_async_copy(src, dst, loc.at[3 + i]) for i, (src, dst) in enumerate(inputs)]
    for c in inputs:
        c.start()
    early = [
        pltpu.make_async_copy(cand_hbm.at[chip_blocks], cand_vm, loc.at[0]),
        pltpu.make_async_copy(logq_hbm.at[chip_blocks], logq_vm, loc.at[1]),
        pltpu.make_async_copy(table_hbm, tab_b, loc.at[2]),
    ]
    for c in early:
        c.start()
    inputs[0].wait()

    lane = lax.broadcasted_iota(I32, (1, LANES), 1)
    halves = range(TOK // HALF)
    tgt = [tgt_ref[q:q + 1, :] for q in halves]
    key = [tgt[q] * TOK + (lane + q * HALF) for q in halves]
    key_col = [column_of(k) for k in key]
    sub = lax.broadcasted_iota(I32, (TOK, LANES), 0)
    hot = [sub == sum(sum_of((key_col[r] < key[q]).astype(I32)) for r in halves) for q in halves]
    perm = jnp.concatenate([jnp.where(h, 1.0, 0.0).astype(BF16) for h in hot], axis=1)
    moved = [jnp.where(hot[q], jnp.broadcast_to(tgt[q].astype(F32), (TOK, LANES)), 0.0) for q in halves]
    my_slot = core * CHIPS + chip
    for r in halves:
        line = sum(sum_of(m[r * HALF:(r + 1) * HALF, :].T) for m in moved)
        tall[row(my_slot), row(r), :] = line.astype(I32).reshape(1, 1, LANES)

    for c in inputs[1:]:
        c.wait()
    xs = dot_nn(perm, x_ref[...]).astype(BF16)
    xs_all[row(chip)] = xs.reshape(1, TOK, IN)
    act = dot_nn(xs, w_in_ref[...])
    u_ref[...] = (act * (0.5 * (1.0 + tanh_of(act)))).astype(BF16)
    hall[row(chip)] = dot_nn(u_ref[...], w_out_ref[...]).astype(BF16).reshape(1, TOK, EMB)

    pl.semaphore_wait(barrier, DEVS - 1)
    tgt_got = to_all(tall, my_slot, tgt_s, tgt_r, slot_of)
    h_got = spread(hall, h_s, h_r, NEAR)
    x_got = spread(xs_all, x_s, x_r, (3, 5, 6, 7))

    for c in early:
        c.wait()
    for r in range(CROW):
        idx_vm[DEVS + r // 2, r % 2:r % 2 + 1, :] = jnp.clip(cand_vm[core, r:r + 1, :] - base, 0, ROWS - 1)
    cand_at = pl.ds(DEVS, CROW // 2)
    cand_copy = pltpu.make_async_copy(idx_vm.at[cand_at], idx_sm.at[cand_at], loc.at[0])
    cand_copy.start()

    @pl.loop(0, ROWS // KC)
    def _(i):
        tab_f[part(i, KC), :] = tab_b[part(i, KC), :].astype(F32)

    tab_f[pl.ds(ROWS, CROW), :] = jnp.zeros((CROW, EMB), F32)
    cand_copy.wait()

    def gather_rows(slot, dst, first):
        for v in range(TOK):
            dst[row(first + v), :] = tab_f[row(idx_sm[slot, v // LANES, v % LANES]), :]

    @pl.loop(0, CAND // TOK)
    def _(i):
        gather_rows(DEVS + i, cand_f, i * TOK)

    e_all[row(core)] = cand_f[...].astype(BF16).reshape(1, CAND, EMB)
    e_copy = swap(e_all.at[core], e_all.at[core], e_s, e_r)

    for c in tgt_got:
        c.wait_recv()
    loc_idx = tall[...] - base
    own = (loc_idx >= 0) & (loc_idx < ROWS)
    idx_vm[0:DEVS] = jnp.where(own, loc_idx, ROWS)

    def count(mask):
        return jnp.sum(jnp.sum(mask.astype(F32), axis=2, keepdims=True), axis=1, keepdims=True)

    lane3 = lax.broadcasted_iota(I32, (DEVS, 1, LANES), 2)
    bounds_vm[...] = jnp.where(lane3 == 0, count(loc_idx < 0), jnp.where(lane3 == 1, count(loc_idx < ROWS // 2), count(loc_idx < ROWS))).astype(I32)
    tok_at = pl.ds(0, DEVS)
    idx_copy = pltpu.make_async_copy(idx_vm.at[tok_at], idx_sm.at[tok_at], loc.at[0])
    idx_copy.start()
    idx_copy.wait()

    @pl.loop(0, CHIPS)
    def _(q):
        gather_rows(oth * CHIPS + q, rows_f, q * TOK)

    trow_s[...] = rows_f[...].astype(BF16)
    tr_copy = swap(trow_s, trow_o, tr_s, tr_r)

    @pl.loop(0, CHIPS)
    def _(q):
        gather_rows(core * CHIPS + q, rows_f, q * TOK)

    for b in range(CORES):
        for r in range(CROW):
            at = b * CAND + r * LANES
            cid_b[at:at + LANES, :] = column_of(cand_vm[b, r:r + 1, :])
            lq_b[at:at + LANES, :] = column_of(logq_vm[b, r:r + 1, :])
    e_copy.wait_recv()
    tr_copy.wait_recv()

    def twice(x):
        return jnp.concatenate([x, x], axis=1)

    def fold(x):
        return x.reshape(PAIR // 8, 8, TOK)

    def stats_of(q):
        h = hall[q]
        ids = tall[core * CHIPS + q]
        y_row = jnp.concatenate([ids[r:r + 1, :] for r in halves], axis=1)

        s = dot_nt(e_all[...].reshape(PAIR, EMB), h) - twice(lq_b[...])
        s = jnp.where(twice(cid_b[...]) == y_row, -1e9, s)
        ex_ref[q] = s
        top = top_of(jnp.max(fold(s), axis=0))
        e = jnp.exp(ex_ref[q] - top)
        ex_ref[q] = e
        tot = sum_of(jnp.sum(fold(e), axis=0))
        rows = rows_f[part(q, TOK), :] + trow_o[part(q, TOK), :].astype(F32)
        tr_t[q] = rows.T
        z = sum_of((rows * h.astype(F32)).T)
        mine = (y_row >= first_row) & (y_row < first_row + CORES * ROWS)
        z_ref[row(q), :] = jnp.where(mine, z, 0.0)
        both = jnp.where(mine, jnp.maximum(top, z), top)
        tot = tot * jnp.exp(top - both) + jnp.where(mine, jnp.exp(jnp.where(mine, z - both, 0.0)), 0.0)
        mloc_ref[row(q), :] = top
        st_all[row(chip), 0, row(q), :] = both.reshape(1, 1, TOK)
        st_all[row(chip), 1, row(q), :] = tot.reshape(1, 1, TOK)

    for pair in ((0, 1), (2, 4), (3, 5), (6, 7)):
        for k in pair:
            if k:
                h_got[k].wait_recv()
        for k in pair:
            stats_of(peers[k] if k else chip)
    st_got = spread(st_all, st_s, st_r, FAR)

    def tower_of(q):
        x = xs_all[q]
        xt_ref[:, part(q, TOK)] = x.T

        act = dot_nn(x, w_in_ref[...])
        tanh = tanh_of(act)
        cdf = 0.5 * (1.0 + tanh)
        slope = cdf + act * (0.5 * (1.0 - tanh * tanh)) * (ROOT_2_PI * (1.0 + 3.0 * CUBE * (act * act)))
        u_t = (act * cdf).astype(BF16).T
        for i in range(HID // LANES):
            tab_f[part(q * (HID // LANES) + i, TOK), :] = slope[:, i * LANES:(i + 1) * LANES]
        for r in halves:
            tab_b[part(q * 2 + r, HID), :] = u_t[:, r * HALF:(r + 1) * HALF]

    for b in range(CORES):
        e_t[:, b * CAND:(b + 1) * CAND] = e_all[b].T
    def late_tower(k):
        x_got[k].wait_recv()
        tower_of(peers[k])

    tower_of(chip)
    for k in TOWERS[:3]:
        late_tower(k)

    for k in NEAR:
        st_got[k].wait_recv()
    top_all = st_all[0, 0]
    for c in range(1, CHIPS):
        top_all = jnp.maximum(top_all, st_all[c, 0])
    tot_all = sum(st_all[c, 1] * jnp.exp(st_all[c, 0] - top_all) for c in range(CHIPS))
    log_norm = top_all + jnp.log(tot_all)
    l_ref[...] = log_norm
    f_ref[...] = jnp.exp(mloc_ref[...] - log_norm) * SHARE
    group = pl.ds(core * CHIPS, CHIPS)
    t_all = jnp.concatenate([tall[group, r, :] for r in halves], axis=1)
    mine_all = (t_all >= first_row) & (t_all < first_row + CORES * ROWS)
    z_all = z_ref[...]
    g_ref[...] = jnp.where(mine_all, (jnp.exp(jnp.where(mine_all, z_all - log_norm, 0.0)) - 1.0) * SHARE, 0.0)
    loss_all[row(me)] = (l_ref[row(chip), :] - sum_of(z_all)).reshape(1, 1, TOK)
    ls_got = to_all(loss_all, me, ls_s, ls_r, lambda device: device)

    def grads_of(q, is_first):
        h = hall[q]
        f_row = f_ref[row(q), :]

        p = (ex_ref[q] * f_row).astype(BF16)
        dh_acc[q] = dot_nn(e_t[...], p) + g_ref[row(q), :] * tr_t[q]
        de = dot_nn(p, h)
        de_acc[...] = de if is_first else de_acc[...] + de

    parts = [pl.ds(r * HALF, HALF) for r in halves]
    JOIN = {7: (1, 6), 6: (2, 4), 5: (4, 1), 3: (1, 2), 4: (4, 0), 1: (1, 0), 2: (2, 0)}

    def pass_on(k, r):
        link = JOIN[k][0]
        go(rcopy(dh_acc.at[peers[k], :, parts[r]], dh_in.at[k, :, parts[r]], dh_s.at[r, k], dh_r.at[r, k], peers[link] * CORES + core))

    def join(k, r):
        link, into = JOIN[k]
        rcopy(dh_in.at[k, :, parts[r]], dh_in.at[k, :, parts[r]], dh_s.at[r, k], dh_r.at[r, k], peers[link] * CORES + core).wait_recv()
        place = peers[into] if into else chip
        dh_acc[place, :, parts[r]] += dh_in[k, :, parts[r]]

    def relay(k, r):
        join(k, r)
        pass_on(JOIN[k][1], r)

    for k in (7, 6, 3, 5, 4):
        grads_of(peers[k], k == FAR[0])
        if k in (7, 3, 5):
            pass_on(k, 0)
            pass_on(k, 1)
    relay(7, 0)
    grads_of(peers[1], False)
    grads_of(peers[2], False)
    relay(7, 1)
    for r in range(2):
        for k in (5, 3, 6):
            relay(k, r)
    grads_of(chip, False)
    de_copy = swap(de_acc.at[part(oth, CAND), :], de_in, de_s, de_r)


    for k in (1, 2, 4):
        go(rcopy(xs_all.at[chip], xs_all.at[chip], x_s.at[k], x_r.at[chip], peers[k] * CORES + core))
    @pl.loop(0, CHIPS)
    def _(q):
        g_row = g_ref[row(q), :]
        for r in halves:
            col = column_of(g_row[:, r * HALF:(r + 1) * HALF])
            gh_ref[part((core * CHIPS + q) * 2 + r, HALF), :] = col * hall[q, r * HALF:(r + 1) * HALF, :].astype(F32)

    gh_copy = swap(gh_ref.at[part(core, GRP), :], gh_ref.at[part(core, GRP), :], gh_s, gh_r)
    late_tower(TOWERS[3])

    db_got = {}
    for r in halves:
        for k in (2, 1, 4):
            join(k, r)
        dhb_all[row(chip), parts[r], :] = dh_acc[chip, :, parts[r]].T.astype(BF16).reshape(1, HALF, EMB)
        for k in DOWN:
            here, there = dhb_all.at[chip, parts[r], :], dhb_all.at[peers[k], parts[r], :]
            dev = peers[k] * CORES + core
            db_got[r, k] = rcopy(there, there, db_s.at[r, k], db_r.at[r, peers[k]], dev)
            go(rcopy(here, here, db_s.at[r, k], db_r.at[r, chip], dev))
    for k in TOWERS[4:]:
        late_tower(k)

    de_copy.wait_recv()
    for r in range(CAND // KC):
        cand_f[r * KC:(r + 1) * KC, :] = de_acc[part(core * (CAND // KC) + r, KC), :] + de_in[r * KC:(r + 1) * KC, :]
    for c in ls_got:
        c.wait_recv()
    loss_out[...] = jnp.sum(jnp.sum(loss_all[...], axis=0), axis=1, keepdims=True) * SHARE
    gh_copy.wait_recv()
    outs = [
        pltpu.make_async_copy(gh_ref, gh_out, loc.at[0]),
        pltpu.make_async_copy(idx_vm, idx_out, loc.at[1]),
        pltpu.make_async_copy(bounds_vm, bounds_out, loc.at[2]),
        pltpu.make_async_copy(cand_f, gcand_out, loc.at[3]),
    ]
    for c in outs:
        c.start()

    def back_of(q):
        dh = dhb_all[q]

        e = dot_nt(dh, w_out_ref[...])
        slope = [tab_f[part(q * (HID // LANES) + i, TOK), :] for i in range(HID // LANES)]
        da_ref[part(q, TOK), :] = (jnp.concatenate(slope, axis=1) * e).astype(BF16)

    w_got = []
    for half, ks in enumerate(((7, 6, 5, 4), (0, 3, 2, 1))):
        for k in ks:
            if k:
                for r in halves:
                    db_got[r, k].wait_recv()
            back_of(peers[k] if k else chip)
        z_side = zc if half else 1 - zc
        xt = xt_ref[:, part(z_side, GRP // 2)]
        for i in range(HSTEPS):
            new = dot_nn(xt, da_ref[part(z_side, GRP // 2), i * HB:(i + 1) * HB])
            gwin[i] = gwin[i] + new if half else new
            if half:
                w_got.append(swap(gwin.at[i], swin.at[i], wi_s.at[i], wi_r.at[i]))
        near = CHIPS // 2
        dh_flat = dhb_all[pl.ds(z_side * near, near)].reshape(GRP // 2, EMB)
        for i in range(HSTEPS):
            at = [((z_side * near + q) * 2 + r) * HID + i * HB for q in range(near) for r in halves]
            u_t = jnp.concatenate([tab_b[pl.ds(pl.multiple_of(a, HB), HB), :] for a in at], axis=1)
            new = dot_nn(u_t, dh_flat)
            here = gwout.at[i * HB:(i + 1) * HB, :]
            here[...] = here[...] + new if half else new
            if half:
                w_got.append(swap(here, swout.at[i * HB:(i + 1) * HB, :], wo_s.at[i], wo_r.at[i]))
    for i in range(HSTEPS):
        w_got[i].wait_recv()
        w_got[i].wait_send()
        gwin[i] += swin[i]
        outs.append(pltpu.make_async_copy(gwin.at[i], dwin_out.at[:, part(i, HB)], loc.at[4 + i]))
        outs[-1].start()
    for c in w_got[HSTEPS:]:
        c.wait_recv()
        c.wait_send()
    gwout[...] += swout[...]
    outs.append(pltpu.make_async_copy(gwout, dwout_out, loc.at[4 + HSTEPS]))
    outs[-1].start()

    for c in sent:
        if not any(c is w for w in w_got):
            c.wait_send()
    for c in outs:
        c.wait()


def scatter_kernel(gcand_hbm, gh_hbm, idx_hbm, bounds_hbm, dwin_ref, dwout_ref, grad_out, dwin_out, dwout_out, acc, gcand, gh, idx_sm, bounds_sm, win_b, wout_b, sems):
    ins = [
        pltpu.make_async_copy(src, dst, sems.at[i])
        for i, (src, dst) in enumerate([(idx_hbm, idx_sm), (bounds_hbm, bounds_sm), (gcand_hbm, gcand), (gh_hbm, gh), (dwin_ref, win_b), (dwout_ref, wout_b)])
    ]
    for c in ins:
        c.start()

    @pl.loop(0, ROWS // KC)
    def _(i):
        acc[part(i, KC), :] = jnp.zeros((KC, EMB), F32)

    for c in ins[:3]:
        c.wait()

    @pl.loop(0, CAND // LANES)
    def _(i):
        for v in range(LANES):
            acc[row(idx_sm[DEVS + i // 2, i % 2, v]), :] = gcand[row(i * LANES + v), :]

    for c in ins[3:]:
        c.wait()
    outs = [pltpu.make_async_copy(win_b, dwin_out, sems.at[6]), pltpu.make_async_copy(wout_b, dwout_out, sems.at[7])]
    for c in outs:
        c.start()

    for half in range(2):

        @pl.loop(0, DEVS)
        def _(s):
            def add(i, carry):
                for v in range(CROW):
                    r = idx_sm[s, i >> 4, (i & 15) * CROW + v]
                    acc[row(r), :] += gh[row(s * TOK + i * CROW + v), :]
                return carry

            first, last = bounds_sm[s, 0, half], bounds_sm[s, 0, half + 1]
            first = (first + 7) >> 3 if half else first >> 3
            lax.fori_loop(first, (last + 7) >> 3, add, 0)

        rows = pl.ds(half * (ROWS // 2), ROWS // 2)
        outs.append(pltpu.make_async_copy(acc.at[rows, :], grad_out.at[rows, :], sems.at[8 + half]))
        outs[-1].start()
    for c in outs:
        c.wait()


def solution(mesh):
    def local_step(features, w_in, w_out, table_blk, cand_ids, log_q, targets):
        vmem = pl.BlockSpec(memory_space=pltpu.VMEM)
        hbm = pl.BlockSpec(memory_space=pl.ANY)
        dma = pltpu.SemaphoreType.DMA
        sds = jax.ShapeDtypeStruct

        def v(dtype, *shape):
            return pltpu.VMEM(shape, dtype)

        chips = dma((CHIPS,))
        idx_shape = (DEVS + CROW // 2, 2, LANES)
        loss, gcand, gh, idx, bounds, dwin, dwout = pl.pallas_call(
            main_kernel,
            name="main_kernel",
            out_shape=(
                sds((1, 1), F32), sds((CAND, EMB), F32), sds((TOTAL, EMB), F32),
                sds(idx_shape, I32), sds((DEVS, 1, LANES), I32), sds((IN, HID), F32), sds((HID, EMB), F32),
            ),
            in_specs=[hbm] * 7,
            out_specs=(vmem,) + (hbm,) * 6,
            scratch_shapes=[
                v(BF16, TOK, IN),
                v(BF16, IN, HID),
                v(BF16, HID, EMB),
                v(I32, 2, LANES),
                v(BF16, ROWS, EMB),
                v(F32, ROWS + CROW, EMB),
                v(I32, DEVS, 2, LANES),
                v(I32, *idx_shape),
                pltpu.SMEM(idx_shape, I32),
                v(I32, CORES, CROW, LANES),
                v(F32, CORES, CROW, LANES),
                v(BF16, CHIPS, TOK, IN),
                v(BF16, IN, GRP),
                v(BF16, TOK, HID),
                v(BF16, CHIPS, TOK, EMB),
                v(F32, GRP, EMB),
                v(F32, CAND, EMB),
                v(BF16, CORES, CAND, EMB),
                v(BF16, EMB, PAIR),
                v(I32, PAIR, LANES),
                v(F32, PAIR, LANES),
                v(BF16, GRP, EMB),
                v(BF16, GRP, EMB),
                v(F32, CHIPS, EMB, TOK),
                v(F32, CHIPS, PAIR, TOK),
                v(F32, CHIPS, 2, CHIPS, TOK),
                v(F32, CHIPS, TOK),
                v(F32, CHIPS, TOK),
                v(F32, CHIPS, TOK),
                v(F32, CHIPS, TOK),
                v(F32, CHIPS, TOK),
                v(F32, TOTAL, EMB),
                v(F32, CHIPS, EMB, TOK),
                v(F32, CHIPS, EMB, TOK),
                v(BF16, CHIPS, TOK, EMB),
                v(BF16, GRP, HID),
                v(F32, PAIR, EMB),
                v(F32, CAND, EMB),
                v(F32, HSTEPS, IN, HB),
                v(F32, HID, EMB),
                v(F32, HSTEPS, IN, HB),
                v(F32, HID, EMB),
                v(F32, DEVS, 1, TOK),
                v(I32, DEVS, 1, LANES),
                dma((DEVS - 1,)), dma((DEVS,)),
                chips, chips,
                chips, chips,
                dma, dma,
                dma, dma,
                chips, chips,
                dma((2, CHIPS)), dma((2, CHIPS)),
                dma, dma,
                dma, dma,
                dma((2, CHIPS)), dma((2, CHIPS)),
                dma((HSTEPS,)), dma((HSTEPS,)),
                dma((HSTEPS,)), dma((HSTEPS,)),
                dma((DEVS - 1,)), dma((DEVS,)),
                dma((CROW + HSTEPS,)),
            ],
            compiler_params=pltpu.CompilerParams(collective_id=0, has_side_effects=True, vmem_limit_bytes=VMEM_LIMIT),
        )(features, w_in, w_out, targets.reshape(2, LANES), cand_ids.reshape(DEVS, CROW, LANES), log_q.reshape(DEVS, CROW, LANES), table_blk)
        grad_blk, grad_in, grad_out = pl.pallas_call(
            scatter_kernel,
            name="scatter_kernel",
            out_shape=(sds((ROWS, EMB), F32), sds((IN, HID), F32), sds((HID, EMB), F32)),
            in_specs=[hbm] * 6,
            out_specs=(hbm,) * 3,
            scratch_shapes=[
                v(F32, ROWS + CROW, EMB),
                v(F32, CAND, EMB),
                v(F32, TOTAL, EMB),
                pltpu.SMEM(idx_shape, I32),
                pltpu.SMEM((DEVS, 1, LANES), I32),
                v(F32, IN, HID),
                v(F32, HID, EMB),
                dma((10,)),
            ],
            compiler_params=pltpu.CompilerParams(vmem_limit_bytes=VMEM_LIMIT),
        )(gcand, gh, idx, bounds, dwin, dwout)
        return loss[0, 0], grad_blk, grad_in, grad_out

    return jax.shard_map(local_step, mesh=mesh, in_specs=(P("dp", None), P(), P(), P("dp", None), P(), P(), P("dp")), out_specs=(P(), P("dp", None), P(), P()), check_vma=False)
```

```python
import jax
import jax.numpy as jnp
from jax import lax
from jax.experimental import pallas as pl
from jax.experimental.pallas import tpu as pltpu
from jax.sharding import PartitionSpec as P

F32 = jnp.float32
BF16 = jnp.bfloat16
I32 = jnp.int32
MESH = pl.DeviceIdType.MESH

CORES = 2
CHIPS = 8
DEVS = 16
LANES = 128
TOK = 256
HALF = 128
GRP = 2048
CAND = 1024
PAIR = 2048
CROW = 8
EMB = 128
HID = 1024
IN = 256
ROWS = 16384
TOTAL = 4096
KC = 256
HB = 256
HSTEPS = HID // HB
ROOT_2_PI = 0.7978845608028654
CUBE = 0.044715
SHARE = 1.0 / TOTAL
VMEM_LIMIT = 64 * 1024 * 1024 - 65536

NEAR = (1, 2, 4, 3, 5, 6, 7)
FAR = (7, 6, 5, 3, 4, 2, 1)
DOWN = (7, 6, 5, 4, 3, 2, 1)
TOWERS = (3, 5, 6, 7, 4, 2, 1)


def dot_nt(lhs, rhs):
    return lax.dot_general(lhs, rhs, (((1,), (1,)), ((), ())), preferred_element_type=F32)


def dot_nn(lhs, rhs):
    return jnp.dot(lhs, rhs, preferred_element_type=F32)


def column_of(row):
    return jnp.broadcast_to(row, (LANES, LANES)).T


def top_of(x):
    return jnp.max(x, axis=0, keepdims=True)


def sum_of(x):
    return jnp.sum(x, axis=0, keepdims=True)


def part(i, size):
    return pl.ds(pl.multiple_of(i * size, size), size)


def row(i):
    return pl.ds(i, 1)


def tanh_of(act):
    return jnp.tanh(ROOT_2_PI * (act + CUBE * (act * act * act)))


def main_kernel(
    x_hbm, w_in_hbm, w_out_hbm, tgt_hbm, cand_hbm, logq_hbm, table_hbm,
    loss_out, gcand_out, gh_out, idx_out, bounds_out, dwin_out, dwout_out,
    x_ref, w_in_ref, w_out_ref, tgt_ref, tab_b, tab_f, tall, idx_vm, idx_sm, cand_vm, logq_vm, xs_all, xt_ref, u_ref, hall,
    rows_f, cand_f, e_all, e_t, cid_b, lq_b, trow_s, trow_o, tr_t,
    ex_ref, st_all, mloc_ref, z_ref, l_ref, f_ref, g_ref, gh_ref,
    dh_acc, dh_in, dhb_all, da_ref, de_acc, de_in, gwin, gwout, swin, swout, loss_all, bounds_vm,
    tgt_s, tgt_r, h_s, h_r, x_s, x_r, e_s, e_r, tr_s, tr_r, st_s, st_r, dh_s, dh_r, de_s, de_r, gh_s, gh_r,
    db_s, db_r, wi_s, wi_r, wo_s, wo_r, ls_s, ls_r, loc,
):
    me = lax.axis_index("dp")
    chip = me // CORES
    core = me % CORES
    oth = 1 - core
    sib = chip * CORES + oth
    base = me * ROWS
    zc = chip // (CHIPS // 2)
    first_row = chip * (CORES * ROWS)

    def flip(k):
        out = 0
        for bit in (1, 2, 4):
            out = out + (((chip // bit) + (k // bit)) % 2) * bit
        return out

    peers = {k: flip(k) for k in NEAR}

    def slot_of(device):
        return (device % CORES) * CHIPS + device // CORES

    def rcopy(src, dst, ssem, rsem, dev):
        return pltpu.make_async_remote_copy(src_ref=src, dst_ref=dst, send_sem=ssem, recv_sem=rsem, device_id=(dev,), device_id_type=MESH)

    sent = []

    def go(copy):
        copy.start()
        sent.append(copy)
        return copy

    def swap(src, dst, ssem, rsem):
        return go(rcopy(src, dst, ssem, rsem, sib))

    def arrivals(ref, ssem, rsem):
        return {k: rcopy(ref.at[src], ref.at[src], ssem.at[k], rsem.at[src], src * CORES + core) for k, src in peers.items()}

    def spread(ref, ssem, rsem, ks):
        got = arrivals(ref, ssem, rsem)
        for k in ks:
            go(rcopy(ref.at[chip], ref.at[chip], ssem.at[k], rsem.at[chip], peers[k] * CORES + core))
        return got

    def to_all(ref, slot, ssem, rsem, slots):
        got = []
        for i in range(DEVS - 1):
            src = slots(lax.rem(me + (DEVS - 1) - i, DEVS))
            got.append(rcopy(ref.at[src], ref.at[src], ssem.at[i], rsem.at[src], others[i]))
        for i, dev in enumerate(others):
            go(rcopy(ref.at[slot], ref.at[slot], ssem.at[i], rsem.at[slot], dev))
        return got

    others = [lax.rem(me + k, DEVS) for k in range(1, DEVS)]

    barrier = pltpu.get_barrier_semaphore()
    for dev in others:
        pl.semaphore_signal(barrier, inc=1, device_id=(dev,), device_id_type=MESH)

    chip_blocks = pl.ds(chip * CORES, CORES)
    inputs = [(tgt_hbm, tgt_ref), (x_hbm, x_ref), (w_in_hbm, w_in_ref), (w_out_hbm, w_out_ref)]
    inputs = [pltpu.make_async_copy(src, dst, loc.at[3 + i]) for i, (src, dst) in enumerate(inputs)]
    for c in inputs:
        c.start()
    early = [
        pltpu.make_async_copy(cand_hbm.at[chip_blocks], cand_vm, loc.at[0]),
        pltpu.make_async_copy(logq_hbm.at[chip_blocks], logq_vm, loc.at[1]),
        pltpu.make_async_copy(table_hbm, tab_b, loc.at[2]),
    ]
    for c in early:
        c.start()
    inputs[0].wait()

    lane = lax.broadcasted_iota(I32, (1, LANES), 1)
    halves = range(TOK // HALF)
    tgt = [tgt_ref[q:q + 1, :] for q in halves]
    key = [tgt[q] * TOK + (lane + q * HALF) for q in halves]
    key_col = [column_of(k) for k in key]
    sub = lax.broadcasted_iota(I32, (TOK, LANES), 0)
    hot = [sub == sum(sum_of((key_col[r] < key[q]).astype(I32)) for r in halves) for q in halves]
    perm = jnp.concatenate([jnp.where(h, 1.0, 0.0).astype(BF16) for h in hot], axis=1)
    moved = [jnp.where(hot[q], jnp.broadcast_to(tgt[q].astype(F32), (TOK, LANES)), 0.0) for q in halves]
    my_slot = core * CHIPS + chip
    for r in halves:
        line = sum(sum_of(m[r * HALF:(r + 1) * HALF, :].T) for m in moved)
        tall[row(my_slot), row(r), :] = line.astype(I32).reshape(1, 1, LANES)

    for c in inputs[1:]:
        c.wait()
    xs = dot_nn(perm, x_ref[...]).astype(BF16)
    xs_all[row(chip)] = xs.reshape(1, TOK, IN)
    act = dot_nn(xs, w_in_ref[...])
    u_ref[...] = (act * (0.5 * (1.0 + tanh_of(act)))).astype(BF16)
    hall[row(chip)] = dot_nn(u_ref[...], w_out_ref[...]).astype(BF16).reshape(1, TOK, EMB)

    pl.semaphore_wait(barrier, DEVS - 1)
    tgt_got = to_all(tall, my_slot, tgt_s, tgt_r, slot_of)
    h_got = spread(hall, h_s, h_r, NEAR)
    x_got = spread(xs_all, x_s, x_r, (3, 5, 6, 7))

    for c in early:
        c.wait()
    for r in range(CROW):
        idx_vm[DEVS + r // 2, r % 2:r % 2 + 1, :] = jnp.clip(cand_vm[core, r:r + 1, :] - base, 0, ROWS - 1)
    cand_at = pl.ds(DEVS, CROW // 2)
    cand_copy = pltpu.make_async_copy(idx_vm.at[cand_at], idx_sm.at[cand_at], loc.at[0])
    cand_copy.start()

    @pl.loop(0, ROWS // KC)
    def _(i):
        tab_f[part(i, KC), :] = tab_b[part(i, KC), :].astype(F32)

    tab_f[pl.ds(ROWS, CROW), :] = jnp.zeros((CROW, EMB), F32)
    cand_copy.wait()

    def gather_rows(slot, dst, first):
        for v in range(TOK):
            dst[row(first + v), :] = tab_f[row(idx_sm[slot, v // LANES, v % LANES]), :]

    @pl.loop(0, CAND // TOK)
    def _(i):
        gather_rows(DEVS + i, cand_f, i * TOK)

    e_all[row(core)] = cand_f[...].astype(BF16).reshape(1, CAND, EMB)
    e_copy = swap(e_all.at[core], e_all.at[core], e_s, e_r)

    for c in tgt_got:
        c.wait_recv()
    loc_idx = tall[...] - base
    own = (loc_idx >= 0) & (loc_idx < ROWS)
    idx_vm[0:DEVS] = jnp.where(own, loc_idx, ROWS)

    def count(mask):
        return jnp.sum(jnp.sum(mask.astype(F32), axis=2, keepdims=True), axis=1, keepdims=True)

    lane3 = lax.broadcasted_iota(I32, (DEVS, 1, LANES), 2)
    bounds_vm[...] = jnp.where(lane3 == 0, count(loc_idx < 0), jnp.where(lane3 == 1, count(loc_idx < ROWS // 2), count(loc_idx < ROWS))).astype(I32)
    tok_at = pl.ds(0, DEVS)
    idx_copy = pltpu.make_async_copy(idx_vm.at[tok_at], idx_sm.at[tok_at], loc.at[0])
    idx_copy.start()
    idx_copy.wait()

    @pl.loop(0, CHIPS)
    def _(q):
        gather_rows(oth * CHIPS + q, rows_f, q * TOK)

    trow_s[...] = rows_f[...].astype(BF16)
    tr_copy = swap(trow_s, trow_o, tr_s, tr_r)

    @pl.loop(0, CHIPS)
    def _(q):
        gather_rows(core * CHIPS + q, rows_f, q * TOK)

    for b in range(CORES):
        for r in range(CROW):
            at = b * CAND + r * LANES
            cid_b[at:at + LANES, :] = column_of(cand_vm[b, r:r + 1, :])
            lq_b[at:at + LANES, :] = column_of(logq_vm[b, r:r + 1, :])
    e_copy.wait_recv()
    tr_copy.wait_recv()

    def twice(x):
        return jnp.concatenate([x, x], axis=1)

    def fold(x):
        return x.reshape(PAIR // 8, 8, TOK)

    def stats_of(q):
        h = hall[q]
        ids = tall[core * CHIPS + q]
        y_row = jnp.concatenate([ids[r:r + 1, :] for r in halves], axis=1)

        s = dot_nt(e_all[...].reshape(PAIR, EMB), h) - twice(lq_b[...])
        s = jnp.where(twice(cid_b[...]) == y_row, -1e9, s)
        ex_ref[q] = s
        top = top_of(jnp.max(fold(s), axis=0))
        e = jnp.exp(ex_ref[q] - top)
        ex_ref[q] = e
        tot = sum_of(jnp.sum(fold(e), axis=0))
        rows = rows_f[part(q, TOK), :] + trow_o[part(q, TOK), :].astype(F32)
        tr_t[q] = rows.T
        z = sum_of((rows * h.astype(F32)).T)
        mine = (y_row >= first_row) & (y_row < first_row + CORES * ROWS)
        z_ref[row(q), :] = jnp.where(mine, z, 0.0)
        both = jnp.where(mine, jnp.maximum(top, z), top)
        tot = tot * jnp.exp(top - both) + jnp.where(mine, jnp.exp(jnp.where(mine, z - both, 0.0)), 0.0)
        mloc_ref[row(q), :] = top
        st_all[row(chip), 0, row(q), :] = both.reshape(1, 1, TOK)
        st_all[row(chip), 1, row(q), :] = tot.reshape(1, 1, TOK)

    for pair in ((0, 1), (2, 4), (3, 5), (6, 7)):
        for k in pair:
            if k:
                h_got[k].wait_recv()
        for k in pair:
            stats_of(peers[k] if k else chip)
    st_got = spread(st_all, st_s, st_r, FAR)

    def tower_of(q):
        x = xs_all[q]
        xt_ref[:, part(q, TOK)] = x.T

        act = dot_nn(x, w_in_ref[...])
        wide = ROOT_2_PI + (ROOT_2_PI * CUBE) * (act * act)
        tanh = jnp.tanh(act * wide)
        cdf = 0.5 + 0.5 * tanh
        slope = cdf + (act * (cdf * (1.0 - tanh))) * (3.0 * wide - 2.0 * ROOT_2_PI)
        u_t = (act * cdf).astype(BF16).T
        for i in range(HID // LANES):
            tab_f[part(q * (HID // LANES) + i, TOK), :] = slope[:, i * LANES:(i + 1) * LANES]
        for r in halves:
            tab_b[part(q * 2 + r, HID), :] = u_t[:, r * HALF:(r + 1) * HALF]

    for b in range(CORES):
        e_t[:, b * CAND:(b + 1) * CAND] = e_all[b].T
    def late_tower(k):
        x_got[k].wait_recv()
        tower_of(peers[k])

    tower_of(chip)
    for k in TOWERS[:3]:
        late_tower(k)

    for k in NEAR:
        st_got[k].wait_recv()
    top_all = st_all[0, 0]
    for c in range(1, CHIPS):
        top_all = jnp.maximum(top_all, st_all[c, 0])
    tot_all = sum(st_all[c, 1] * jnp.exp(st_all[c, 0] - top_all) for c in range(CHIPS))
    log_norm = top_all + jnp.log(tot_all)
    l_ref[...] = log_norm
    f_ref[...] = jnp.exp(mloc_ref[...] - log_norm) * SHARE
    group = pl.ds(core * CHIPS, CHIPS)
    t_all = jnp.concatenate([tall[group, r, :] for r in halves], axis=1)
    mine_all = (t_all >= first_row) & (t_all < first_row + CORES * ROWS)
    z_all = z_ref[...]
    g_ref[...] = jnp.where(mine_all, (jnp.exp(jnp.where(mine_all, z_all - log_norm, 0.0)) - 1.0) * SHARE, 0.0)
    loss_all[row(me)] = (l_ref[row(chip), :] - sum_of(z_all)).reshape(1, 1, TOK)
    ls_got = to_all(loss_all, me, ls_s, ls_r, lambda device: device)

    def grads_of(q, is_first):
        h = hall[q]
        f_row = f_ref[row(q), :]

        p = (ex_ref[q] * f_row).astype(BF16)
        dh_acc[q] = dot_nn(e_t[...], p) + g_ref[row(q), :] * tr_t[q]
        de = dot_nn(p, h)
        de_acc[...] = de if is_first else de_acc[...] + de

    parts = [pl.ds(r * HALF, HALF) for r in halves]
    JOIN = {7: (1, 6), 6: (2, 4), 5: (4, 1), 3: (1, 2), 4: (4, 0), 1: (1, 0), 2: (2, 0)}

    def pass_on(k, r):
        link = JOIN[k][0]
        go(rcopy(dh_acc.at[peers[k], :, parts[r]], dh_in.at[k, :, parts[r]], dh_s.at[r, k], dh_r.at[r, k], peers[link] * CORES + core))

    def join(k, r):
        link, into = JOIN[k]
        rcopy(dh_in.at[k, :, parts[r]], dh_in.at[k, :, parts[r]], dh_s.at[r, k], dh_r.at[r, k], peers[link] * CORES + core).wait_recv()
        place = peers[into] if into else chip
        dh_acc[place, :, parts[r]] += dh_in[k, :, parts[r]]

    def relay(k, r):
        join(k, r)
        pass_on(JOIN[k][1], r)

    for k in (7, 6, 3, 5, 4):
        grads_of(peers[k], k == FAR[0])
        if k in (7, 3, 5):
            pass_on(k, 0)
            pass_on(k, 1)
    relay(7, 0)
    grads_of(peers[1], False)
    grads_of(peers[2], False)
    relay(7, 1)
    for r in range(2):
        for k in (5, 3, 6):
            relay(k, r)
    grads_of(chip, False)
    de_copy = swap(de_acc.at[part(oth, CAND), :], de_in, de_s, de_r)


    for k in (1, 2, 4):
        go(rcopy(xs_all.at[chip], xs_all.at[chip], x_s.at[k], x_r.at[chip], peers[k] * CORES + core))
    @pl.loop(0, CHIPS)
    def _(q):
        g_row = g_ref[row(q), :]
        for r in halves:
            col = column_of(g_row[:, r * HALF:(r + 1) * HALF])
            gh_ref[part((core * CHIPS + q) * 2 + r, HALF), :] = col * hall[q, r * HALF:(r + 1) * HALF, :].astype(F32)

    gh_copy = swap(gh_ref.at[part(core, GRP), :], gh_ref.at[part(core, GRP), :], gh_s, gh_r)
    late_tower(TOWERS[3])

    db_got = {}
    for r in halves:
        for k in (2, 1, 4):
            join(k, r)
        dhb_all[row(chip), parts[r], :] = dh_acc[chip, :, parts[r]].T.astype(BF16).reshape(1, HALF, EMB)
        for k in DOWN:
            here, there = dhb_all.at[chip, parts[r], :], dhb_all.at[peers[k], parts[r], :]
            dev = peers[k] * CORES + core
            db_got[r, k] = rcopy(there, there, db_s.at[r, k], db_r.at[r, peers[k]], dev)
            go(rcopy(here, here, db_s.at[r, k], db_r.at[r, chip], dev))
    for k in TOWERS[4:]:
        late_tower(k)

    de_copy.wait_recv()
    for r in range(CAND // KC):
        cand_f[r * KC:(r + 1) * KC, :] = de_acc[part(core * (CAND // KC) + r, KC), :] + de_in[r * KC:(r + 1) * KC, :]
    for c in ls_got:
        c.wait_recv()
    loss_out[...] = jnp.sum(jnp.sum(loss_all[...], axis=0), axis=1, keepdims=True) * SHARE
    gh_copy.wait_recv()
    outs = [
        pltpu.make_async_copy(gh_ref, gh_out, loc.at[0]),
        pltpu.make_async_copy(idx_vm, idx_out, loc.at[1]),
        pltpu.make_async_copy(bounds_vm, bounds_out, loc.at[2]),
        pltpu.make_async_copy(cand_f, gcand_out, loc.at[3]),
    ]
    for c in outs:
        c.start()

    def back_of(q):
        dh = dhb_all[q]

        e = dot_nt(dh, w_out_ref[...])
        slope = [tab_f[part(q * (HID // LANES) + i, TOK), :] for i in range(HID // LANES)]
        da_ref[part(q, TOK), :] = (jnp.concatenate(slope, axis=1) * e).astype(BF16)

    w_got = []
    for half, ks in enumerate(((7, 6, 5, 4), (0, 3, 2, 1))):
        for k in ks:
            if k:
                for r in halves:
                    db_got[r, k].wait_recv()
            back_of(peers[k] if k else chip)
        z_side = zc if half else 1 - zc
        xt = xt_ref[:, part(z_side, GRP // 2)]
        for i in range(HSTEPS):
            new = dot_nn(xt, da_ref[part(z_side, GRP // 2), i * HB:(i + 1) * HB])
            gwin[i] = gwin[i] + new if half else new
            if half:
                w_got.append(swap(gwin.at[i], swin.at[i], wi_s.at[i], wi_r.at[i]))
        near = CHIPS // 2
        dh_flat = dhb_all[pl.ds(z_side * near, near)].reshape(GRP // 2, EMB)
        for i in range(HSTEPS):
            at = [((z_side * near + q) * 2 + r) * HID + i * HB for q in range(near) for r in halves]
            u_t = jnp.concatenate([tab_b[pl.ds(pl.multiple_of(a, HB), HB), :] for a in at], axis=1)
            new = dot_nn(u_t, dh_flat)
            here = gwout.at[i * HB:(i + 1) * HB, :]
            here[...] = here[...] + new if half else new
            if half:
                w_got.append(swap(here, swout.at[i * HB:(i + 1) * HB, :], wo_s.at[i], wo_r.at[i]))
    for i in range(HSTEPS):
        w_got[i].wait_recv()
        w_got[i].wait_send()
        gwin[i] += swin[i]
        outs.append(pltpu.make_async_copy(gwin.at[i], dwin_out.at[:, part(i, HB)], loc.at[4 + i]))
        outs[-1].start()
    for c in w_got[HSTEPS:]:
        c.wait_recv()
        c.wait_send()
    gwout[...] += swout[...]
    outs.append(pltpu.make_async_copy(gwout, dwout_out, loc.at[4 + HSTEPS]))
    outs[-1].start()

    for c in sent:
        if not any(c is w for w in w_got):
            c.wait_send()
    for c in outs:
        c.wait()


def scatter_kernel(gcand_hbm, gh_hbm, idx_hbm, bounds_hbm, dwin_ref, dwout_ref, grad_out, dwin_out, dwout_out, acc, gcand, gh, idx_sm, bounds_sm, win_b, wout_b, sems):
    ins = [
        pltpu.make_async_copy(src, dst, sems.at[i])
        for i, (src, dst) in enumerate([(idx_hbm, idx_sm), (bounds_hbm, bounds_sm), (gcand_hbm, gcand), (gh_hbm, gh), (dwin_ref, win_b), (dwout_ref, wout_b)])
    ]
    for c in ins:
        c.start()

    @pl.loop(0, ROWS // KC)
    def _(i):
        acc[part(i, KC), :] = jnp.zeros((KC, EMB), F32)

    for c in ins[:3]:
        c.wait()

    @pl.loop(0, CAND // LANES)
    def _(i):
        for v in range(LANES):
            acc[row(idx_sm[DEVS + i // 2, i % 2, v]), :] = gcand[row(i * LANES + v), :]

    for c in ins[3:]:
        c.wait()
    outs = [pltpu.make_async_copy(win_b, dwin_out, sems.at[6]), pltpu.make_async_copy(wout_b, dwout_out, sems.at[7])]
    for c in outs:
        c.start()

    for half in range(2):

        @pl.loop(0, DEVS)
        def _(s):
            def add(i, carry):
                for v in range(CROW):
                    r = idx_sm[s, i >> 4, (i & 15) * CROW + v]
                    acc[row(r), :] += gh[row(s * TOK + i * CROW + v), :]
                return carry

            first, last = bounds_sm[s, 0, half], bounds_sm[s, 0, half + 1]
            first = (first + 7) >> 3 if half else first >> 3
            lax.fori_loop(first, (last + 7) >> 3, add, 0)

        rows = pl.ds(half * (ROWS // 2), ROWS // 2)
        outs.append(pltpu.make_async_copy(acc.at[rows, :], grad_out.at[rows, :], sems.at[8 + half]))
        outs[-1].start()
    for c in outs:
        c.wait()


def solution(mesh):
    def local_step(features, w_in, w_out, table_blk, cand_ids, log_q, targets):
        vmem = pl.BlockSpec(memory_space=pltpu.VMEM)
        hbm = pl.BlockSpec(memory_space=pl.ANY)
        dma = pltpu.SemaphoreType.DMA
        sds = jax.ShapeDtypeStruct

        def v(dtype, *shape):
            return pltpu.VMEM(shape, dtype)

        chips = dma((CHIPS,))
        idx_shape = (DEVS + CROW // 2, 2, LANES)
        loss, gcand, gh, idx, bounds, dwin, dwout = pl.pallas_call(
            main_kernel,
            name="main_kernel",
            out_shape=(
                sds((1, 1), F32), sds((CAND, EMB), F32), sds((TOTAL, EMB), F32),
                sds(idx_shape, I32), sds((DEVS, 1, LANES), I32), sds((IN, HID), F32), sds((HID, EMB), F32),
            ),
            in_specs=[hbm] * 7,
            out_specs=(vmem,) + (hbm,) * 6,
            scratch_shapes=[
                v(BF16, TOK, IN),
                v(BF16, IN, HID),
                v(BF16, HID, EMB),
                v(I32, 2, LANES),
                v(BF16, ROWS, EMB),
                v(F32, ROWS + CROW, EMB),
                v(I32, DEVS, 2, LANES),
                v(I32, *idx_shape),
                pltpu.SMEM(idx_shape, I32),
                v(I32, CORES, CROW, LANES),
                v(F32, CORES, CROW, LANES),
                v(BF16, CHIPS, TOK, IN),
                v(BF16, IN, GRP),
                v(BF16, TOK, HID),
                v(BF16, CHIPS, TOK, EMB),
                v(F32, GRP, EMB),
                v(F32, CAND, EMB),
                v(BF16, CORES, CAND, EMB),
                v(BF16, EMB, PAIR),
                v(I32, PAIR, LANES),
                v(F32, PAIR, LANES),
                v(BF16, GRP, EMB),
                v(BF16, GRP, EMB),
                v(F32, CHIPS, EMB, TOK),
                v(F32, CHIPS, PAIR, TOK),
                v(F32, CHIPS, 2, CHIPS, TOK),
                v(F32, CHIPS, TOK),
                v(F32, CHIPS, TOK),
                v(F32, CHIPS, TOK),
                v(F32, CHIPS, TOK),
                v(F32, CHIPS, TOK),
                v(F32, TOTAL, EMB),
                v(F32, CHIPS, EMB, TOK),
                v(F32, CHIPS, EMB, TOK),
                v(BF16, CHIPS, TOK, EMB),
                v(BF16, GRP, HID),
                v(F32, PAIR, EMB),
                v(F32, CAND, EMB),
                v(F32, HSTEPS, IN, HB),
                v(F32, HID, EMB),
                v(F32, HSTEPS, IN, HB),
                v(F32, HID, EMB),
                v(F32, DEVS, 1, TOK),
                v(I32, DEVS, 1, LANES),
                dma((DEVS - 1,)), dma((DEVS,)),
                chips, chips,
                chips, chips,
                dma, dma,
                dma, dma,
                chips, chips,
                dma((2, CHIPS)), dma((2, CHIPS)),
                dma, dma,
                dma, dma,
                dma((2, CHIPS)), dma((2, CHIPS)),
                dma((HSTEPS,)), dma((HSTEPS,)),
                dma((HSTEPS,)), dma((HSTEPS,)),
                dma((DEVS - 1,)), dma((DEVS,)),
                dma((CROW + HSTEPS,)),
            ],
            compiler_params=pltpu.CompilerParams(collective_id=0, has_side_effects=True, vmem_limit_bytes=VMEM_LIMIT),
        )(features, w_in, w_out, targets.reshape(2, LANES), cand_ids.reshape(DEVS, CROW, LANES), log_q.reshape(DEVS, CROW, LANES), table_blk)
        grad_blk, grad_in, grad_out = pl.pallas_call(
            scatter_kernel,
            name="scatter_kernel",
            out_shape=(sds((ROWS, EMB), F32), sds((IN, HID), F32), sds((HID, EMB), F32)),
            in_specs=[hbm] * 6,
            out_specs=(hbm,) * 3,
            scratch_shapes=[
                v(F32, ROWS + CROW, EMB),
                v(F32, CAND, EMB),
                v(F32, TOTAL, EMB),
                pltpu.SMEM(idx_shape, I32),
                pltpu.SMEM((DEVS, 1, LANES), I32),
                v(F32, IN, HID),
                v(F32, HID, EMB),
                dma((10,)),
            ],
            compiler_params=pltpu.CompilerParams(vmem_limit_bytes=VMEM_LIMIT),
        )(gcand, gh, idx, bounds, dwin, dwout)
        return loss[0, 0], grad_blk, grad_in, grad_out

    return jax.shard_map(local_step, mesh=mesh, in_specs=(P("dp", None), P(), P(), P("dp", None), P(), P(), P("dp")), out_specs=(P(), P("dp", None), P(), P()), check_vma=False)
```
